1024 devices in a mesh: gx: 32 (over z_lo, core), gy: 8 (over z_hi, x), gz: 4 (over y).
Axes of the slice: x: 4, y: 4, z: 32 (z_hi: 2, z_lo: 16; z = z_hi * 16 + z_lo), core: 2. Of those that a mesh axis runs over, the one named last changes fastest.
Arguments:
- conserved_state: float32 [6, 128, 64, 480], P(None, 'gx', 'gy', 'gz'), as said below
Outputs:
- updated_state: float32 [6, 128, 64, 480], P(None, 'gx', 'gy', 'gz')
- next_timestep: float32 [], replicated
Inputs may be any that keep to these rules, and one draw needn't show every extreme that they name: `conserved_state`: component 0 is density within 0.5 to 3, components 1 to 3 are density times velocities each within -1 to 1, component 4 is total energy with pressure within 0.5 to 6, component 5 is density times a tracer fraction within 0 to 1.
All inputs are finite; a program needn't handle non-finite values.
Results may differ from the reference program's by a relative error of at most 0.0003.
Values sent between devices are 32-bit elements; how exact they have to be, the bound alone decides.
No kernel may reach another device: no remote copies, remote signals or barrier semaphores. Data moves between devices by JAX's collectives and lax.ppermute only.
A program may use at most 32 MiB of HBM per device.

```python
import math
import jax
import jax.numpy as jnp
from jax import lax

CX = 4
GHOST = 4
NX = 128
NY = 64
NZ = 480


def draw_conserved_state(key, part):
    subkeys = jax.random.split(key, 6)
    grid_shape = (NX, NY, NZ)
    across = lax.broadcasted_iota(jnp.float32, grid_shape, 0) / NX
    density = jnp.exp(jax.random.uniform(subkeys[0], grid_shape, jnp.float32, math.log(0.5), math.log(2.0)))
    pressure = jnp.exp(jax.random.uniform(subkeys[1], grid_shape, jnp.float32, math.log(0.5), math.log(2.0)))
    tracer = jax.random.uniform(subkeys[5], grid_shape, jnp.float32, 0.0, 1.0)
    pressure = pressure * (1.0 + 2.0 * across)
    velocity = [jnp.clip(0.25 * jax.random.normal(subkeys[component], grid_shape, jnp.float32), -1.0, 1.0) for component in (2, 3, 4)]
    kinetic = 0.5 * density * (velocity[0] * velocity[0] + velocity[1] * velocity[1] + velocity[2] * velocity[2])
    energy = pressure / (5.0 / 3.0 - 1.0) + kinetic
    return jnp.stack([density, density * velocity[0], density * velocity[1], density * velocity[2], energy, density * tracer]).astype(jnp.float32)


def setup_inputs(seed: int = 0) -> dict:
    keys = jax.random.split(jax.random.key(seed), 2)
    return {
        "conserved_state": draw_conserved_state(jax.random.fold_in(keys[1], 71), 0),
    }


adiabatic = 5.0 / 3.0
courant = 0.3

def shifted(values, sweep_axis, offset):
    return jnp.roll(values, -offset, axis=sweep_axis)

def primitive_of(conserved_list):
    density = conserved_list[0]
    inverse = 1.0 / density
    velocity = [conserved_list[component] * inverse for component in (1, 2, 3)]
    kinetic = 0.5 * (conserved_list[1] * velocity[0] + conserved_list[2] * velocity[1] + conserved_list[3] * velocity[2])
    pressure = (adiabatic - 1.0) * (conserved_list[4] - kinetic)
    return [density, velocity[0], velocity[1], velocity[2], pressure, conserved_list[5] * inverse]

def conserved_of(primitive):
    density = primitive[0]
    momenta = [density * primitive[component] for component in (1, 2, 3)]
    kinetic = 0.5 * (momenta[0] * primitive[1] + momenta[1] * primitive[2] + momenta[2] * primitive[3])
    energy = primitive[4] / (adiabatic - 1.0) + kinetic
    return [density, momenta[0], momenta[1], momenta[2], energy, density * primitive[5]]

def fastest_signal(conserved_list):
    primitive = primitive_of(conserved_list)
    sound = jnp.sqrt(adiabatic * primitive[4] / primitive[0])
    speeds = jnp.maximum(jnp.maximum(jnp.abs(primitive[1]), jnp.abs(primitive[2])), jnp.abs(primitive[3]))
    return jnp.max(speeds + sound)

def parabola(centre, sweep_axis):
    before_one = shifted(centre, sweep_axis, -1)
    before_two = shifted(centre, sweep_axis, -2)
    before_three = shifted(centre, sweep_axis, -3)
    after_one = shifted(centre, sweep_axis, 1)
    after_two = shifted(centre, sweep_axis, 2)
    edge = (37.0 * (before_one + centre) - 8.0 * (before_two + after_one) + (before_three + after_two)) / 60.0
    edge = jnp.clip(edge, jnp.minimum(before_one, centre), jnp.maximum(before_one, centre))
    lower = edge
    upper = shifted(edge, sweep_axis, 1)
    flatten = (upper - centre) * (centre - lower) <= 0.0
    spread = upper - lower
    skewed = spread * (centre - 0.5 * (lower + upper))
    limit = spread * spread / 6.0
    new_lower = jnp.where(flatten, centre, jnp.where(skewed > limit, 3.0 * centre - 2.0 * upper, lower))
    new_upper = jnp.where(flatten, centre, jnp.where(skewed < -limit, 3.0 * centre - 2.0 * lower, upper))
    return (new_lower, new_upper)

def traced_faces(primitive, sweep_axis, time_step):
    normal = 1 + sweep_axis
    edges = [parabola(item, sweep_axis) for item in primitive]
    slopes = [pair[1] - pair[0] for pair in edges]
    normal_vel = primitive[normal]
    density = primitive[0]
    rates = [-(normal_vel * slopes[0] + density * slopes[normal])]
    for component in (1, 2, 3):
        if component == normal:
            rates.append(-(normal_vel * slopes[normal] + slopes[4] / density))
        else:
            rates.append(-normal_vel * slopes[component])
    rates.append(-(adiabatic * primitive[4] * slopes[normal] + normal_vel * slopes[4]))
    rates.append(-normal_vel * slopes[5])
    lower_faces = [edges[component][0] + 0.5 * time_step * rates[component] for component in range(6)]
    upper_faces = [edges[component][1] + 0.5 * time_step * rates[component] for component in range(6)]
    return (lower_faces, upper_faces)

def physical_flux(primitive, conserved_list, normal):
    normal_vel = primitive[normal]
    result = [item * normal_vel for item in conserved_list]
    result[normal] = result[normal] + primitive[4]
    result[4] = result[4] + primitive[4] * normal_vel
    return result

def star_state(primitive, conserved_list, outer_speed, middle_speed, normal):
    mass_rate = primitive[0] * (outer_speed - primitive[normal])
    factor = mass_rate / (outer_speed - middle_speed)
    result = [factor * primitive[component] for component in range(6)]
    result[0] = factor
    result[normal] = factor * middle_speed
    result[4] = factor * (conserved_list[4] / primitive[0] + (middle_speed - primitive[normal]) * (middle_speed + primitive[4] / mass_rate))
    return result

def hllc_flux(left, right, sweep_axis):
    normal = 1 + sweep_axis
    sound_left = jnp.sqrt(adiabatic * left[4] / left[0])
    sound_right = jnp.sqrt(adiabatic * right[4] / right[0])
    low_speed = jnp.minimum(left[normal] - sound_left, right[normal] - sound_right)
    high_speed = jnp.maximum(left[normal] + sound_left, right[normal] + sound_right)
    mass_left = left[0] * (low_speed - left[normal])
    mass_right = right[0] * (high_speed - right[normal])
    middle = (right[4] - left[4] + mass_left * left[normal] - mass_right * right[normal]) / (mass_left - mass_right)
    left_state = conserved_of(left)
    right_state = conserved_of(right)
    flux_left = physical_flux(left, left_state, normal)
    flux_right = physical_flux(right, right_state, normal)
    star_left = star_state(left, left_state, low_speed, middle, normal)
    star_right = star_state(right, right_state, high_speed, middle, normal)
    result = []
    for component in range(6):
        left_star_flux = flux_left[component] + low_speed * (star_left[component] - left_state[component])
        right_star_flux = flux_right[component] + high_speed * (star_right[component] - right_state[component])
        chosen = jnp.where(high_speed > 0.0, right_star_flux, flux_right[component])
        chosen = jnp.where(middle >= 0.0, left_star_flux, chosen)
        chosen = jnp.where(low_speed >= 0.0, flux_left[component], chosen)
        result.append(chosen)
    return result

def hydro_step(padded, time_step):
    conserved_list = [padded[component] for component in range(6)]
    primitive = primitive_of(conserved_list)
    faces = [traced_faces(primitive, sweep_axis, time_step) for sweep_axis in range(3)]
    predicted = []
    for sweep_axis in range(3):
        lower_faces, upper_faces = faces[sweep_axis]
        from_below = [shifted(item, sweep_axis, -1) for item in upper_faces]
        predicted.append(hllc_flux(from_below, lower_faces, sweep_axis))
    final_fluxes = []
    for sweep_axis in range(3):
        lower_faces, upper_faces = faces[sweep_axis]
        lower_state = conserved_of(lower_faces)
        upper_state = conserved_of(upper_faces)
        for other_axis in range(3):
            if other_axis != sweep_axis:
                for component in range(6):
                    flux_other = predicted[other_axis][component]
                    divergence = 0.5 * time_step * (shifted(flux_other, other_axis, 1) - flux_other)
                    lower_state[component] = lower_state[component] - divergence
                    upper_state[component] = upper_state[component] - divergence
        lower_prim = primitive_of(lower_state)
        upper_prim = primitive_of(upper_state)
        from_below = [shifted(item, sweep_axis, -1) for item in upper_prim]
        final_fluxes.append(hllc_flux(from_below, lower_prim, sweep_axis))
    updated = []
    for component in range(6):
        total = conserved_list[component]
        for sweep_axis in range(3):
            flux_here = final_fluxes[sweep_axis][component]
            total = total - time_step * (shifted(flux_here, sweep_axis, 1) - flux_here)
        updated.append(total[GHOST:-GHOST, GHOST:-GHOST, GHOST:-GHOST])
    return jnp.stack(updated)

def reference(conserved_state):
    slab_count = NX // CX
    indices = jnp.arange(slab_count).astype(jnp.int32)

    def slab_signal(slab_index):
        slab = lax.dynamic_slice_in_dim(conserved_state, slab_index * CX, CX, 1)
        return fastest_signal([slab[component] for component in range(6)])
    signal_now = jnp.max(lax.map(slab_signal, indices))
    time_step = courant / signal_now

    def slab_update(slab_index):
        plane_rows = (slab_index * CX - GHOST + jnp.arange(CX + 2 * GHOST).astype(jnp.int32)) % NX
        slab = jnp.take(conserved_state, plane_rows.astype(jnp.int32), axis=1)
        padded = jnp.pad(slab, ((0, 0), (0, 0), (GHOST, GHOST), (GHOST, GHOST)), mode='wrap')
        updated = hydro_step(padded, time_step)
        return (updated, fastest_signal([updated[component] for component in range(6)]))
    blocks, signals = lax.map(slab_update, indices)
    updated_state = jnp.transpose(blocks, (1, 0, 2, 3, 4)).reshape(6, NX, NY, NZ)
    next_timestep = courant / jnp.max(signals)
    return (updated_state, next_timestep)
```

```python
import jax
import jax.numpy as jnp
from jax import lax
from jax.sharding import Mesh
from jax.sharding import PartitionSpec as P

GHOST = 4
ALL = ("zl", "c", "zh", "x", "y")
PLANE = ("c", "x", "y")
COLUMN = ("zl", "zh")
GX = ("zl", "c")
GY = ("zh", "x")
GZ = ("y",)

adiabatic = 5.0 / 3.0
courant = 0.3


def over_all(value):
    for axes in (PLANE, COLUMN):
        count = lax.axis_size(axes)
        everyone = lax.all_to_all(jnp.broadcast_to(value, (count,)), axes, 0, 0, tiled=True)
        value = jnp.max(everyone)
    return value


def swaps(count):
    even = [(i, i ^ 1) for i in range(count)]
    odd = [(i, (i + 1) % count if i % 2 else (i - 1) % count) for i in range(count)]
    return even, odd


def exchange(block, axes, parity, dim, width):
    even, odd = swaps(lax.axis_size(axes))
    first = lax.slice_in_dim(block, 0, width, axis=dim)
    last = lax.slice_in_dim(block, block.shape[dim] - width, None, axis=dim)
    if block.shape[dim] == width:
        to_even, to_odd = block, block
    else:
        to_even, to_odd = jnp.where(parity, first, last), jnp.where(parity, last, first)
    by_even = lax.ppermute(to_even, axes, even)
    by_odd = lax.ppermute(to_odd, axes, odd)
    return jnp.where(parity, by_even, by_odd), jnp.where(parity, by_odd, by_even)


def padded(block, axes, parity, dim, width):
    low, high = exchange(block, axes, parity, dim, width)
    return jnp.concatenate([low, block, high], axis=dim)


def window(values, axis_number, start, length):
    return lax.slice_in_dim(values, start, start + length, axis=axis_number)


def primitive_of(conserved_list):
    density = conserved_list[0]
    inverse = 1.0 / density
    velocity = [conserved_list[component] * inverse for component in (1, 2, 3)]
    kinetic = 0.5 * (
        conserved_list[1] * velocity[0]
        + conserved_list[2] * velocity[1]
        + conserved_list[3] * velocity[2]
    )
    pressure = (adiabatic - 1.0) * (conserved_list[4] - kinetic)
    return [density, velocity[0], velocity[1], velocity[2], pressure, conserved_list[5] * inverse]


def conserved_of(primitive):
    density = primitive[0]
    momenta = [density * primitive[component] for component in (1, 2, 3)]
    kinetic = 0.5 * (
        momenta[0] * primitive[1] + momenta[1] * primitive[2] + momenta[2] * primitive[3]
    )
    energy = primitive[4] / (adiabatic - 1.0) + kinetic
    return [density, momenta[0], momenta[1], momenta[2], energy, density * primitive[5]]


def fastest_signal(conserved_list):
    primitive = primitive_of(conserved_list)
    sound = jnp.sqrt(adiabatic * primitive[4] / primitive[0])
    speeds = jnp.maximum(
        jnp.maximum(jnp.abs(primitive[1]), jnp.abs(primitive[2])), jnp.abs(primitive[3])
    )
    return jnp.max(speeds + sound)


def parabola(centre, sweep_axis):
    extent = centre.shape[sweep_axis]
    count = extent - 5

    def offset_cells(offset):
        return window(centre, sweep_axis, 3 + offset, count)

    before_one = offset_cells(-1)
    middle = offset_cells(0)
    edge = (
        37.0 * (before_one + middle)
        - 8.0 * (offset_cells(-2) + offset_cells(1))
        + (offset_cells(-3) + offset_cells(2))
    ) / 60.0
    edge = jnp.clip(edge, jnp.minimum(before_one, middle), jnp.maximum(before_one, middle))
    lower = window(edge, sweep_axis, 0, count - 1)
    upper = window(edge, sweep_axis, 1, count - 1)
    inner = window(centre, sweep_axis, 3, count - 1)
    flatten = (upper - inner) * (inner - lower) <= 0.0
    spread = upper - lower
    skewed = spread * (inner - 0.5 * (lower + upper))
    limit = spread * spread / 6.0
    new_lower = jnp.where(
        flatten, inner, jnp.where(skewed > limit, 3.0 * inner - 2.0 * upper, lower)
    )
    new_upper = jnp.where(
        flatten, inner, jnp.where(skewed < -limit, 3.0 * inner - 2.0 * lower, upper)
    )
    return (new_lower, new_upper)


def traced_faces(primitive, sweep_axis, time_step):
    normal = 1 + sweep_axis
    extent = primitive[0].shape[sweep_axis]
    edges = [parabola(item, sweep_axis) for item in primitive]
    slopes = [pair[1] - pair[0] for pair in edges]
    inner = [window(item, sweep_axis, 3, extent - 6) for item in primitive]
    normal_vel = inner[normal]
    density = inner[0]
    rates = [-(normal_vel * slopes[0] + density * slopes[normal])]
    for component in (1, 2, 3):
        if component == normal:
            rates.append(-(normal_vel * slopes[normal] + slopes[4] / density))
        else:
            rates.append(-normal_vel * slopes[component])
    rates.append(-(adiabatic * inner[4] * slopes[normal] + normal_vel * slopes[4]))
    rates.append(-normal_vel * slopes[5])
    lower_faces = [
        edges[component][0] + 0.5 * time_step * rates[component] for component in range(6)
    ]
    upper_faces = [
        edges[component][1] + 0.5 * time_step * rates[component] for component in range(6)
    ]
    return (lower_faces, upper_faces)


def physical_flux(primitive, conserved_list, normal):
    normal_vel = primitive[normal]
    result = [item * normal_vel for item in conserved_list]
    result[normal] = result[normal] + primitive[4]
    result[4] = result[4] + primitive[4] * normal_vel
    return result


def star_state(primitive, conserved_list, outer_speed, middle_speed, normal):
    mass_rate = primitive[0] * (outer_speed - primitive[normal])
    factor = mass_rate / (outer_speed - middle_speed)
    result = [factor * primitive[component] for component in range(6)]
    result[0] = factor
    result[normal] = factor * middle_speed
    result[4] = factor * (
        conserved_list[4] / primitive[0]
        + (middle_speed - primitive[normal]) * (middle_speed + primitive[4] / mass_rate)
    )
    return result


def hllc_flux(left, right, sweep_axis):
    normal = 1 + sweep_axis
    sound_left = jnp.sqrt(adiabatic * left[4] / left[0])
    sound_right = jnp.sqrt(adiabatic * right[4] / right[0])
    low_speed = jnp.minimum(left[normal] - sound_left, right[normal] - sound_right)
    high_speed = jnp.maximum(left[normal] + sound_left, right[normal] + sound_right)
    mass_left = left[0] * (low_speed - left[normal])
    mass_right = right[0] * (high_speed - right[normal])
    middle = (right[4] - left[4] + mass_left * left[normal] - mass_right * right[normal]) / (
        mass_left - mass_right
    )
    left_state = conserved_of(left)
    right_state = conserved_of(right)
    flux_left = physical_flux(left, left_state, normal)
    flux_right = physical_flux(right, right_state, normal)
    star_left = star_state(left, left_state, low_speed, middle, normal)
    star_right = star_state(right, right_state, high_speed, middle, normal)
    result = []
    for component in range(6):
        left_star_flux = flux_left[component] + low_speed * (
            star_left[component] - left_state[component]
        )
        right_star_flux = flux_right[component] + high_speed * (
            star_right[component] - right_state[component]
        )
        chosen = jnp.where(high_speed > 0.0, right_star_flux, flux_right[component])
        chosen = jnp.where(middle >= 0.0, left_star_flux, chosen)
        chosen = jnp.where(low_speed >= 0.0, flux_left[component], chosen)
        result.append(chosen)
    return result


def face_fluxes(lower_faces, upper_faces, sweep_axis):
    extent = lower_faces[0].shape[sweep_axis]
    from_below = [window(item, sweep_axis, 0, extent - 1) for item in upper_faces]
    from_above = [window(item, sweep_axis, 1, extent - 1) for item in lower_faces]
    return hllc_flux(from_below, from_above, sweep_axis)


def hydro_step(padded, time_step):
    conserved_list = [padded[component] for component in range(6)]
    extents = padded.shape[1:]
    owned = [extent - 2 * GHOST for extent in extents]
    primitive = primitive_of(conserved_list)
    faces = [traced_faces(primitive, sweep_axis, time_step) for sweep_axis in range(3)]
    predicted = [
        face_fluxes(faces[sweep_axis][0], faces[sweep_axis][1], sweep_axis)
        for sweep_axis in range(3)
    ]
    final_fluxes = []
    for sweep_axis in range(3):
        lower_faces, upper_faces = faces[sweep_axis]
        lower_state = conserved_of(lower_faces)
        upper_state = conserved_of(upper_faces)
        for other_axis in range(3):
            if other_axis != sweep_axis:
                for component in range(6):
                    lower_state[component] = window(
                        lower_state[component], other_axis, GHOST, owned[other_axis]
                    )
                    upper_state[component] = window(
                        upper_state[component], other_axis, GHOST, owned[other_axis]
                    )
        for other_axis in range(3):
            if other_axis != sweep_axis:
                for component in range(6):
                    flux_other = predicted[other_axis][component]
                    divergence = (
                        0.5
                        * time_step
                        * (
                            window(flux_other, other_axis, 1, owned[other_axis])
                            - window(flux_other, other_axis, 0, owned[other_axis])
                        )
                    )
                    for third_axis in range(3):
                        if third_axis == sweep_axis:
                            divergence = window(divergence, third_axis, 3, extents[third_axis] - 6)
                        elif third_axis != other_axis:
                            divergence = window(divergence, third_axis, GHOST, owned[third_axis])
                    lower_state[component] = lower_state[component] - divergence
                    upper_state[component] = upper_state[component] - divergence
        lower_prim = primitive_of(lower_state)
        upper_prim = primitive_of(upper_state)
        final_fluxes.append(face_fluxes(lower_prim, upper_prim, sweep_axis))
    updated = []
    for component in range(6):
        total = conserved_list[component][GHOST:-GHOST, GHOST:-GHOST, GHOST:-GHOST]
        for sweep_axis in range(3):
            flux_here = final_fluxes[sweep_axis][component]
            total = total - time_step * (
                window(flux_here, sweep_axis, 1, owned[sweep_axis])
                - window(flux_here, sweep_axis, 0, owned[sweep_axis])
            )
        updated.append(total)
    return jnp.stack(updated)


def body(conserved_state):
    own_cells = [conserved_state[component] for component in range(6)]
    signal_now = over_all(fastest_signal(own_cells))
    time_step = courant / signal_now
    block = padded(conserved_state, GZ, lax.axis_index("y") % 2 == 1, 3, GHOST)
    block = padded(block, GY, lax.axis_index("x") % 2 == 1, 2, GHOST)
    block = padded(block, GX, lax.axis_index("c") == 1, 1, GHOST)
    updated = hydro_step(block, time_step)
    new_cells = [updated[component] for component in range(6)]
    signal_next = over_all(fastest_signal(new_cells))
    return (updated, courant / signal_next)


def solution(mesh):
    finer = Mesh(mesh.devices.reshape(16, 2, 2, 4, 4), ALL)
    spec = P(None, GX, GY, GZ)
    return jax.shard_map(
        body, mesh=finer, in_specs=(spec,), out_specs=(spec, P()), check_vma=False
    )
```

```python
import jax
import jax.numpy as jnp
from jax import lax
from jax.sharding import Mesh
from jax.sharding import PartitionSpec as P

GHOST = 4
ALL = ("zl", "c", "zh", "x", "y")
PLANE = ("c", "x", "y")
COLUMN = ("zl", "zh")
GX = ("zl", "c")
GY = ("zh", "x")
GZ = ("y",)

adiabatic = 5.0 / 3.0
courant = 0.3


def over_group(value, axes):
    everyone = lax.all_to_all(
        jnp.broadcast_to(value, (lax.axis_size(axes),)), axes, 0, 0, tiled=True
    )
    return jnp.max(everyone)


def swaps(count):
    even = [(i, i ^ 1) for i in range(count)]
    odd = [(i, (i + 1) % count if i % 2 else (i - 1) % count) for i in range(count)]
    return even, odd


def padded(block, axes, parity, dim, width):
    even, odd = swaps(lax.axis_size(axes))
    first = lax.slice_in_dim(block, 0, width, axis=dim)
    last = lax.slice_in_dim(block, block.shape[dim] - width, None, axis=dim)
    if block.shape[dim] == width:
        to_even, to_odd = block, block
    else:
        to_even, to_odd = jnp.where(parity, first, last), jnp.where(parity, last, first)
    by_odd = lax.ppermute(to_odd, axes, odd)
    by_even = lax.ppermute(to_even, axes, even)
    low, high = jnp.where(parity, by_even, by_odd), jnp.where(parity, by_odd, by_even)
    return jnp.concatenate([low, block, high], axis=dim)


def window(values, axis_number, start, length):
    return lax.slice_in_dim(values, start, start + length, axis=axis_number)


def primitive_of(conserved_list):
    density = conserved_list[0]
    inverse = 1.0 / density
    velocity = [conserved_list[component] * inverse for component in (1, 2, 3)]
    kinetic = 0.5 * (
        conserved_list[1] * velocity[0]
        + conserved_list[2] * velocity[1]
        + conserved_list[3] * velocity[2]
    )
    pressure = (adiabatic - 1.0) * (conserved_list[4] - kinetic)
    return [density, velocity[0], velocity[1], velocity[2], pressure, conserved_list[5] * inverse]


def conserved_of(primitive):
    density = primitive[0]
    momenta = [density * primitive[component] for component in (1, 2, 3)]
    kinetic = 0.5 * (
        momenta[0] * primitive[1] + momenta[1] * primitive[2] + momenta[2] * primitive[3]
    )
    energy = primitive[4] / (adiabatic - 1.0) + kinetic
    return [density, momenta[0], momenta[1], momenta[2], energy, density * primitive[5]]


def fastest_signal(conserved_list):
    primitive = primitive_of(conserved_list)
    sound = jnp.sqrt(adiabatic * primitive[4] / primitive[0])
    speeds = jnp.maximum(
        jnp.maximum(jnp.abs(primitive[1]), jnp.abs(primitive[2])), jnp.abs(primitive[3])
    )
    return jnp.max(speeds + sound)


def parabola(centre, sweep_axis):
    extent = centre.shape[sweep_axis]
    count = extent - 5

    def offset_cells(offset):
        return window(centre, sweep_axis, 3 + offset, count)

    before_one = offset_cells(-1)
    middle = offset_cells(0)
    edge = (
        37.0 * (before_one + middle)
        - 8.0 * (offset_cells(-2) + offset_cells(1))
        + (offset_cells(-3) + offset_cells(2))
    ) / 60.0
    edge = jnp.clip(edge, jnp.minimum(before_one, middle), jnp.maximum(before_one, middle))
    lower = window(edge, sweep_axis, 0, count - 1)
    upper = window(edge, sweep_axis, 1, count - 1)
    inner = window(centre, sweep_axis, 3, count - 1)
    flatten = (upper - inner) * (inner - lower) <= 0.0
    spread = upper - lower
    skewed = spread * (inner - 0.5 * (lower + upper))
    limit = spread * spread / 6.0
    new_lower = jnp.where(
        flatten, inner, jnp.where(skewed > limit, 3.0 * inner - 2.0 * upper, lower)
    )
    new_upper = jnp.where(
        flatten, inner, jnp.where(skewed < -limit, 3.0 * inner - 2.0 * lower, upper)
    )
    return (new_lower, new_upper)


def traced_faces(primitive, sweep_axis, time_step):
    normal = 1 + sweep_axis
    extent = primitive[0].shape[sweep_axis]
    edges = [parabola(item, sweep_axis) for item in primitive]
    slopes = [pair[1] - pair[0] for pair in edges]
    inner = [window(item, sweep_axis, 3, extent - 6) for item in primitive]
    normal_vel = inner[normal]
    density = inner[0]
    rates = [-(normal_vel * slopes[0] + density * slopes[normal])]
    for component in (1, 2, 3):
        if component == normal:
            rates.append(-(normal_vel * slopes[normal] + slopes[4] / density))
        else:
            rates.append(-normal_vel * slopes[component])
    rates.append(-(adiabatic * inner[4] * slopes[normal] + normal_vel * slopes[4]))
    rates.append(-normal_vel * slopes[5])
    lower_faces = [
        edges[component][0] + 0.5 * time_step * rates[component] for component in range(6)
    ]
    upper_faces = [
        edges[component][1] + 0.5 * time_step * rates[component] for component in range(6)
    ]
    return (lower_faces, upper_faces)


def physical_flux(primitive, conserved_list, normal):
    normal_vel = primitive[normal]
    result = [item * normal_vel for item in conserved_list]
    result[normal] = result[normal] + primitive[4]
    result[4] = result[4] + primitive[4] * normal_vel
    return result


def star_state(primitive, conserved_list, outer_speed, middle_speed, normal):
    mass_rate = primitive[0] * (outer_speed - primitive[normal])
    factor = mass_rate / (outer_speed - middle_speed)
    result = [factor * primitive[component] for component in range(6)]
    result[0] = factor
    result[normal] = factor * middle_speed
    result[4] = factor * (
        conserved_list[4] / primitive[0]
        + (middle_speed - primitive[normal]) * (middle_speed + primitive[4] / mass_rate)
    )
    return result


def hllc_flux(left, right, sweep_axis):
    normal = 1 + sweep_axis
    sound_left = jnp.sqrt(adiabatic * left[4] / left[0])
    sound_right = jnp.sqrt(adiabatic * right[4] / right[0])
    low_speed = jnp.minimum(left[normal] - sound_left, right[normal] - sound_right)
    high_speed = jnp.maximum(left[normal] + sound_left, right[normal] + sound_right)
    mass_left = left[0] * (low_speed - left[normal])
    mass_right = right[0] * (high_speed - right[normal])
    middle = (right[4] - left[4] + mass_left * left[normal] - mass_right * right[normal]) / (
        mass_left - mass_right
    )
    left_state = conserved_of(left)
    right_state = conserved_of(right)
    flux_left = physical_flux(left, left_state, normal)
    flux_right = physical_flux(right, right_state, normal)
    star_left = star_state(left, left_state, low_speed, middle, normal)
    star_right = star_state(right, right_state, high_speed, middle, normal)
    result = []
    for component in range(6):
        left_star_flux = flux_left[component] + low_speed * (
            star_left[component] - left_state[component]
        )
        right_star_flux = flux_right[component] + high_speed * (
            star_right[component] - right_state[component]
        )
        chosen = jnp.where(high_speed > 0.0, right_star_flux, flux_right[component])
        chosen = jnp.where(middle >= 0.0, left_star_flux, chosen)
        chosen = jnp.where(low_speed >= 0.0, flux_left[component], chosen)
        result.append(chosen)
    return result


def face_fluxes(lower_faces, upper_faces, sweep_axis):
    extent = lower_faces[0].shape[sweep_axis]
    from_below = [window(item, sweep_axis, 0, extent - 1) for item in upper_faces]
    from_above = [window(item, sweep_axis, 1, extent - 1) for item in lower_faces]
    return hllc_flux(from_below, from_above, sweep_axis)


def hydro_step(padded, time_step):
    conserved_list = [padded[component] for component in range(6)]
    extents = padded.shape[1:]
    owned = [extent - 2 * GHOST for extent in extents]
    primitive = primitive_of(conserved_list)
    faces = [traced_faces(primitive, sweep_axis, time_step) for sweep_axis in range(3)]
    predicted = [
        face_fluxes(faces[sweep_axis][0], faces[sweep_axis][1], sweep_axis)
        for sweep_axis in range(3)
    ]
    final_fluxes = []
    for sweep_axis in range(3):
        lower_faces, upper_faces = faces[sweep_axis]
        lower_state = conserved_of(lower_faces)
        upper_state = conserved_of(upper_faces)
        for other_axis in range(3):
            if other_axis != sweep_axis:
                for component in range(6):
                    lower_state[component] = window(
                        lower_state[component], other_axis, GHOST, owned[other_axis]
                    )
                    upper_state[component] = window(
                        upper_state[component], other_axis, GHOST, owned[other_axis]
                    )
        for other_axis in range(3):
            if other_axis != sweep_axis:
                for component in range(6):
                    flux_other = predicted[other_axis][component]
                    divergence = (
                        0.5
                        * time_step
                        * (
                            window(flux_other, other_axis, 1, owned[other_axis])
                            - window(flux_other, other_axis, 0, owned[other_axis])
                        )
                    )
                    for third_axis in range(3):
                        if third_axis == sweep_axis:
                            divergence = window(divergence, third_axis, 3, extents[third_axis] - 6)
                        elif third_axis != other_axis:
                            divergence = window(divergence, third_axis, GHOST, owned[third_axis])
                    lower_state[component] = lower_state[component] - divergence
                    upper_state[component] = upper_state[component] - divergence
        lower_prim = primitive_of(lower_state)
        upper_prim = primitive_of(upper_state)
        final_fluxes.append(face_fluxes(lower_prim, upper_prim, sweep_axis))
    updated = []
    for component in range(6):
        total = conserved_list[component][GHOST:-GHOST, GHOST:-GHOST, GHOST:-GHOST]
        for sweep_axis in range(3):
            flux_here = final_fluxes[sweep_axis][component]
            total = total - time_step * (
                window(flux_here, sweep_axis, 1, owned[sweep_axis])
                - window(flux_here, sweep_axis, 0, owned[sweep_axis])
            )
        updated.append(total)
    return jnp.stack(updated)


def step(conserved_state):
    own_cells = [conserved_state[component] for component in range(6)]
    signal_now = fastest_signal(own_cells)
    block = padded(conserved_state, GZ, lax.axis_index("y") % 2 == 1, 3, GHOST)
    signal_now = over_group(signal_now, PLANE)
    block = padded(block, GY, lax.axis_index("x") % 2 == 1, 2, GHOST)
    signal_now = over_group(signal_now, COLUMN)
    block = padded(block, GX, lax.axis_index("c") == 1, 1, GHOST)
    time_step = courant / signal_now
    updated = hydro_step(block, time_step)
    new_cells = [updated[component] for component in range(6)]
    signal_next = fastest_signal(new_cells)
    signal_next = over_group(signal_next, PLANE)
    signal_next = over_group(signal_next, COLUMN)
    return (updated, courant / signal_next)


def solution(mesh):
    finer = Mesh(mesh.devices.reshape(16, 2, 2, 4, 4), ALL)
    spec = P(None, GX, GY, GZ)
    return jax.shard_map(step, mesh=finer, in_specs=(spec,), out_specs=(spec, P()), check_vma=False)
```

```python
import jax
import jax.numpy as jnp
from jax import lax
from jax.experimental import pallas as pl
from jax.experimental.pallas import tpu as pltpu
from jax.sharding import Mesh
from jax.sharding import PartitionSpec as P

GHOST = 4
ALL = ("zl", "c", "zh", "x", "y")
PLANE = ("c", "x", "y")
COLUMN = ("zl", "zh")
GX = ("zl", "c")
GY = ("zh", "x")
GZ = ("y",)

adiabatic = 5.0 / 3.0
courant = 0.3


def over_group(value, axes):
    everyone = lax.all_to_all(
        jnp.broadcast_to(value, (lax.axis_size(axes),)), axes, 0, 0, tiled=True
    )
    return jnp.max(everyone)


def swaps(count):
    even = [(i, i ^ 1) for i in range(count)]
    odd = [(i, (i + 1) % count if i % 2 else (i - 1) % count) for i in range(count)]
    return even, odd


def ghosts(block, axes, parity, dim, width):
    even, odd = swaps(lax.axis_size(axes))
    first = lax.slice_in_dim(block, 0, width, axis=dim)
    last = lax.slice_in_dim(block, block.shape[dim] - width, None, axis=dim)
    if block.shape[dim] == width:
        to_even, to_odd = block, block
    else:
        to_even, to_odd = jnp.where(parity, first, last), jnp.where(parity, last, first)
    by_odd = lax.ppermute(to_odd, axes, odd)
    by_even = lax.ppermute(to_even, axes, even)
    return jnp.where(parity, by_even, by_odd), jnp.where(parity, by_odd, by_even)


def padded(block, axes, parity, dim, width):
    low, high = ghosts(block, axes, parity, dim, width)
    return jnp.concatenate([block, high, low], axis=dim)


def roll(value, shift, axis):
    return pltpu.roll(value, shift % value.shape[axis], axis)


def primitive_of(conserved):
    density, energy = conserved[0], conserved[4]
    inverse = 1.0 / density
    speed = [conserved[component] * inverse for component in (1, 2, 3)]
    kinetic = 0.5 * (conserved[1] * speed[0] + conserved[2] * speed[1] + conserved[3] * speed[2])
    return [density, *speed, (adiabatic - 1.0) * (energy - kinetic), conserved[5] * inverse]


def conserved_of(primitive):
    density = primitive[0]
    momenta = [density * primitive[component] for component in (1, 2, 3)]
    kinetic = 0.5 * (
        momenta[0] * primitive[1] + momenta[1] * primitive[2] + momenta[2] * primitive[3]
    )
    energy = primitive[4] * (1.0 / (adiabatic - 1.0)) + kinetic
    return [density, *momenta, energy, density * primitive[5]]


def fastest_signal(conserved):
    primitive = primitive_of(conserved)
    sound = jnp.sqrt(adiabatic * primitive[4] / primitive[0])
    speeds = jnp.maximum(
        jnp.maximum(jnp.abs(primitive[1]), jnp.abs(primitive[2])), jnp.abs(primitive[3])
    )
    return speeds + sound


def edge_of(q3, q2, q1, q, a1, a2):
    edge = (37.0 / 60.0) * (q1 + q) - (8.0 / 60.0) * (q2 + a1) + (1.0 / 60.0) * (q3 + a2)
    return jnp.clip(edge, jnp.minimum(q1, q), jnp.maximum(q1, q))


def limited(q, lower, upper):
    above, below = upper - q, q - lower
    spread = upper - lower
    skewed = spread * (0.5 * (below - above))
    limit = spread * spread * (1.0 / 6.0)
    flat = above * below <= 0.0
    new_lower = jnp.where(flat, q, jnp.where(skewed > limit, q - 2.0 * above, lower))
    new_upper = jnp.where(flat, q, jnp.where(skewed < -limit, q + 2.0 * below, upper))
    return new_lower, new_upper


def traced(primitive, edges, normal, half_step):
    slopes = [upper - lower for lower, upper in edges]
    density, speed, pressure = primitive[0], primitive[normal], primitive[4]
    rates = [-(speed * slopes[component]) for component in range(6)]
    rates[0] = rates[0] - density * slopes[normal]
    rates[normal] = rates[normal] - slopes[4] / density
    rates[4] = rates[4] - adiabatic * pressure * slopes[normal]
    moves = [half_step * rate for rate in rates]
    lower = [edges[component][0] + moves[component] for component in range(6)]
    upper = [edges[component][1] + moves[component] for component in range(6)]
    return lower, upper


def hllc_flux(left, right, normal):
    ratio_left, ratio_right = left[4] / left[0], right[4] / right[0]
    sound_left, sound_right = jnp.sqrt(adiabatic * ratio_left), jnp.sqrt(adiabatic * ratio_right)
    low = jnp.minimum(left[normal] - sound_left, right[normal] - sound_right)
    high = jnp.maximum(left[normal] + sound_left, right[normal] + sound_right)
    mass_left = left[0] * (low - left[normal])
    mass_right = right[0] * (high - right[normal])
    middle = (right[4] - left[4] + mass_left * left[normal] - mass_right * right[normal]) / (
        mass_left - mass_right
    )
    from_left = middle >= 0.0
    side = [jnp.where(from_left, left[component], right[component]) for component in range(6)]
    ratio = jnp.where(from_left, ratio_left, ratio_right)
    mass = jnp.where(from_left, mass_left, mass_right)
    outer = jnp.where(from_left, low, high)
    weight = jnp.where(from_left, jnp.minimum(low, 0.0), jnp.maximum(high, 0.0))
    speed, pressure = side[normal], side[4]
    state = conserved_of(side)
    flux = [item * speed for item in state]
    flux[normal] = flux[normal] + pressure
    flux[4] = flux[4] + pressure * speed
    factor = mass / (outer - middle)
    star = [factor * item for item in side]
    star[0] = factor
    star[normal] = factor * middle
    half_square = 0.5 * (side[1] * side[1] + side[2] * side[2] + side[3] * side[3])
    specific = ratio * (1.0 / (adiabatic - 1.0)) + half_square
    star[4] = factor * (specific + (middle - speed) * (middle + pressure / mass))
    return [flux[c] + weight * (star[c] - state[c]) for c in range(6)]


def kernel(step_ref, low_ref, own_ref, high_ref, out_ref, signal_ref, prim, lower, upper, fluxes, gx):
    step = step_ref[0]
    half = 0.5 * step
    for source, start in ((low_ref, 0), (own_ref, 4), (high_ref, 8)):
        for layer in range(4):
            values = primitive_of([source[c, layer] for c in range(6)])
            for c in range(6):
                prim[c, start + layer] = values[c]

    def faces(index, carry):
        own = [prim[c, index + 3] for c in range(6)]
        edges = []
        for c in range(6):
            q = [prim[c, index + k] for k in range(7)]
            edges.append(
                limited(own[c], edge_of(*q[0:6]), edge_of(*q[1:7]))
            )
        for axis in range(3):
            if axis:
                edges = []
                for c in range(6):
                    q = own[c]
                    near = [roll(q, k, axis - 1) for k in (3, 2, 1)]
                    far = [roll(q, -k, axis - 1) for k in (1, 2)]
                    edge = edge_of(*near, q, *far)
                    edges.append(limited(q, edge, roll(edge, -1, axis - 1)))
            low_face, high_face = traced(own, edges, 1 + axis, half)
            for c in range(6):
                lower[axis, c, index] = low_face[c]
                upper[axis, c, index] = high_face[c]
        return carry

    lax.fori_loop(0, 6, faces, 0)

    def predicted(index, carry):
        for axis in (1, 2):
            left = [roll(upper[axis, c, index], 1, axis - 1) for c in range(6)]
            flux = hllc_flux(left, [lower[axis, c, index] for c in range(6)], 1 + axis)
            for c in range(6):
                fluxes[axis, c, index] = half * (roll(flux[c], -1, axis - 1) - flux[c])
        return carry

    lax.fori_loop(0, 6, predicted, 0)

    def predicted_first(index, carry):
        flux = hllc_flux(
            [upper[0, c, index] for c in range(6)], [lower[0, c, index + 1] for c in range(6)], 1
        )
        for c in range(6):
            fluxes[0, c, index] = flux[c]
        return carry

    lax.fori_loop(0, 5, predicted_first, 0)

    def corrected(states, changes):
        state = conserved_of(states)
        return primitive_of([state[c] - changes[c] for c in range(6)])

    def final_first(index, carry):
        change = [fluxes[1, c, index + 1, 0:8] + fluxes[2, c, index + 1, 0:8] for c in range(6)]
        before = [carry[c] for c in range(6)]
        right = corrected([lower[0, c, index + 1, 0:8] for c in range(6)], change)
        flux = hllc_flux(before, right, 1)
        for c in range(6):
            gx[c, index] = flux[c]
        return tuple(corrected([upper[0, c, index + 1, 0:8] for c in range(6)], change))

    change = [fluxes[1, c, 0, 0:8] + fluxes[2, c, 0, 0:8] for c in range(6)]
    first = tuple(corrected([upper[0, c, 0, 0:8] for c in range(6)], change))
    lax.fori_loop(0, 5, final_first, first)

    lanes = lax.broadcasted_iota(jnp.int32, (8, 128), 1) < 120

    def final(index, fastest):
        here = index + 1
        total = [own_ref[c, index, 0:8] - step * (gx[c, index + 1] - gx[c, index]) for c in range(6)]
        ahead = [half * (fluxes[0, c, here] - fluxes[0, c, index]) for c in range(6)]
        change = [ahead[c] + fluxes[2, c, here] for c in range(6)]
        left = corrected([upper[1, c, here] for c in range(6)], change)
        right = corrected([lower[1, c, here] for c in range(6)], change)
        flux = hllc_flux([roll(item, 1, 0) for item in left], right, 2)
        total = [total[c] - step * (roll(flux[c], -1, 0)[0:8] - flux[c][0:8]) for c in range(6)]
        change = [ahead[c][0:8] + fluxes[1, c, here, 0:8] for c in range(6)]
        left = corrected([upper[2, c, here, 0:8] for c in range(6)], change)
        right = corrected([lower[2, c, here, 0:8] for c in range(6)], change)
        flux = hllc_flux([roll(item, 1, 1) for item in left], right, 3)
        total = [total[c] - step * (roll(flux[c], -1, 1) - flux[c]) for c in range(6)]
        for c in range(6):
            out_ref[c, index] = total[c][:, 0:120]
        return jnp.maximum(fastest, jnp.where(lanes, fastest_signal(total), 0.0))

    fastest = lax.fori_loop(0, 4, final, jnp.zeros((8, 128), jnp.float32))
    signal_ref[0] = jnp.max(fastest)


def hydro_step(low, own, high, time_step):
    vmem = pl.BlockSpec(memory_space=pltpu.VMEM)
    smem = pl.BlockSpec(memory_space=pltpu.SMEM)
    return pl.pallas_call(
        kernel,
        in_specs=[smem, vmem, vmem, vmem],
        out_specs=[vmem, smem],
        out_shape=[
            jax.ShapeDtypeStruct((6, 4, 8, 120), jnp.float32),
            jax.ShapeDtypeStruct((1,), jnp.float32),
        ],
        scratch_shapes=[
            pltpu.VMEM((6, 12, 16, 128), jnp.float32),
            pltpu.VMEM((3, 6, 6, 16, 128), jnp.float32),
            pltpu.VMEM((3, 6, 6, 16, 128), jnp.float32),
            pltpu.VMEM((3, 6, 6, 16, 128), jnp.float32),
            pltpu.VMEM((6, 5, 8, 128), jnp.float32),
        ],
        name="hydro",
    )(time_step.reshape(1), low, own, high)


def step(conserved_state):
    signal_now = jnp.max(fastest_signal([conserved_state[component] for component in range(6)]))
    block = padded(conserved_state, GZ, lax.axis_index("y") % 2 == 1, 3, GHOST)
    signal_now = over_group(signal_now, PLANE)
    block = padded(block, GY, lax.axis_index("x") % 2 == 1, 2, GHOST)
    block, signal_now = lax.optimization_barrier((block, signal_now))
    signal_now = over_group(signal_now, COLUMN)
    low, high = ghosts(block, GX, lax.axis_index("c") == 1, 1, GHOST)
    updated, signal_next = hydro_step(low, block, high, courant / signal_now)
    signal_next = over_group(signal_next[0], PLANE)
    signal_next = over_group(signal_next, COLUMN)
    return (updated, courant / signal_next)


def solution(mesh):
    finer = Mesh(mesh.devices.reshape(16, 2, 2, 4, 4), ALL)
    spec = P(None, GX, GY, GZ)
    return jax.shard_map(step, mesh=finer, in_specs=(spec,), out_specs=(spec, P()), check_vma=False)
```

```python
import jax
import jax.numpy as jnp
from jax import lax
from jax.experimental import pallas as pl
from jax.experimental.pallas import tpu as pltpu
from jax.sharding import Mesh
from jax.sharding import PartitionSpec as P

GHOST = 4
ALL = ("zl", "c", "zh", "x", "y")
PLANE = ("c", "x", "y")
COLUMN = ("zl", "zh")
GX = ("zl", "c")
GY = ("zh", "x")
GZ = ("y",)

adiabatic = 5.0 / 3.0
courant = 0.3


def over_group(value, axes):
    everyone = lax.all_to_all(
        jnp.broadcast_to(value, (lax.axis_size(axes),)), axes, 0, 0, tiled=True
    )
    return jnp.max(everyone)


def over_column(value, first):
    halves, rows = lax.axis_size("zh"), lax.axis_size("zl")
    deep = halves * rows
    order = [(first + step) % deep for step in range(deep)]
    columns, width = lax.axis_size("c"), lax.axis_size(("x", "y"))
    groups = [
        [(((z % rows) * columns + c) * halves + z // rows) * width + place for z in order]
        for c in range(columns)
        for place in range(width)
    ]
    everyone = lax.all_to_all(
        jnp.broadcast_to(value, (deep,)), ALL, 0, 0, axis_index_groups=groups, tiled=True
    )
    return jnp.max(everyone)


def swaps(count):
    even = [(i, i ^ 1) for i in range(count)]
    odd = [(i, (i + 1) % count if i % 2 else (i - 1) % count) for i in range(count)]
    return even, odd


def ghosts(block, axes, parity, dim, width):
    even, odd = swaps(lax.axis_size(axes))
    first = lax.slice_in_dim(block, 0, width, axis=dim)
    last = lax.slice_in_dim(block, block.shape[dim] - width, None, axis=dim)
    if block.shape[dim] == width:
        to_even, to_odd = block, block
    else:
        to_even, to_odd = jnp.where(parity, first, last), jnp.where(parity, last, first)
    by_odd = lax.ppermute(to_odd, axes, odd)
    by_even = lax.ppermute(to_even, axes, even)
    return jnp.where(parity, by_even, by_odd), jnp.where(parity, by_odd, by_even)


def padded(block, axes, parity, dim, width):
    low, high = ghosts(block, axes, parity, dim, width)
    return jnp.concatenate([block, high, low], axis=dim)


def roll(value, shift, axis):
    return pltpu.roll(value, shift % value.shape[axis], axis)


def primitive_of(conserved):
    density, energy = conserved[0], conserved[4]
    inverse = 1.0 / density
    speed = [conserved[component] * inverse for component in (1, 2, 3)]
    kinetic = 0.5 * (conserved[1] * speed[0] + conserved[2] * speed[1] + conserved[3] * speed[2])
    return [density, *speed, (adiabatic - 1.0) * (energy - kinetic), conserved[5] * inverse]


def conserved_of(primitive):
    density = primitive[0]
    momenta = [density * primitive[component] for component in (1, 2, 3)]
    kinetic = 0.5 * (
        momenta[0] * primitive[1] + momenta[1] * primitive[2] + momenta[2] * primitive[3]
    )
    energy = primitive[4] * (1.0 / (adiabatic - 1.0)) + kinetic
    return [density, *momenta, energy, density * primitive[5]]


def fastest_signal(conserved):
    primitive = primitive_of(conserved)
    sound = jnp.sqrt(adiabatic * primitive[4] / primitive[0])
    speeds = jnp.maximum(
        jnp.maximum(jnp.abs(primitive[1]), jnp.abs(primitive[2])), jnp.abs(primitive[3])
    )
    return speeds + sound


def edge_of(q3, q2, q1, q, a1, a2):
    edge = (37.0 / 60.0) * (q1 + q) - (8.0 / 60.0) * (q2 + a1) + (1.0 / 60.0) * (q3 + a2)
    return jnp.clip(edge, jnp.minimum(q1, q), jnp.maximum(q1, q))


def limited(q, lower, upper):
    above, below = upper - q, q - lower
    spread = upper - lower
    skewed = spread * (0.5 * (below - above))
    limit = spread * spread * (1.0 / 6.0)
    flat = above * below <= 0.0
    new_lower = jnp.where(flat, q, jnp.where(skewed > limit, q - 2.0 * above, lower))
    new_upper = jnp.where(flat, q, jnp.where(skewed < -limit, q + 2.0 * below, upper))
    return new_lower, new_upper


def traced(primitive, edges, normal, half_step):
    slopes = [upper - lower for lower, upper in edges]
    density, speed, pressure = primitive[0], primitive[normal], primitive[4]
    rates = [-(speed * slopes[component]) for component in range(6)]
    rates[0] = rates[0] - density * slopes[normal]
    rates[normal] = rates[normal] - slopes[4] / density
    rates[4] = rates[4] - adiabatic * pressure * slopes[normal]
    moves = [half_step * rate for rate in rates]
    lower = [edges[component][0] + moves[component] for component in range(6)]
    upper = [edges[component][1] + moves[component] for component in range(6)]
    return lower, upper


def hllc_flux(left, right, normal):
    ratio_left, ratio_right = left[4] / left[0], right[4] / right[0]
    sound_left, sound_right = jnp.sqrt(adiabatic * ratio_left), jnp.sqrt(adiabatic * ratio_right)
    low = jnp.minimum(left[normal] - sound_left, right[normal] - sound_right)
    high = jnp.maximum(left[normal] + sound_left, right[normal] + sound_right)
    mass_left = left[0] * (low - left[normal])
    mass_right = right[0] * (high - right[normal])
    middle = (right[4] - left[4] + mass_left * left[normal] - mass_right * right[normal]) / (
        mass_left - mass_right
    )
    from_left = middle >= 0.0
    side = [jnp.where(from_left, left[component], right[component]) for component in range(6)]
    ratio = jnp.where(from_left, ratio_left, ratio_right)
    mass = jnp.where(from_left, mass_left, mass_right)
    outer = jnp.where(from_left, low, high)
    weight = jnp.where(from_left, jnp.minimum(low, 0.0), jnp.maximum(high, 0.0))
    speed, pressure = side[normal], side[4]
    state = conserved_of(side)
    flux = [item * speed for item in state]
    flux[normal] = flux[normal] + pressure
    flux[4] = flux[4] + pressure * speed
    factor = mass / (outer - middle)
    star = [factor * item for item in side]
    star[0] = factor
    star[normal] = factor * middle
    half_square = 0.5 * (side[1] * side[1] + side[2] * side[2] + side[3] * side[3])
    specific = ratio * (1.0 / (adiabatic - 1.0)) + half_square
    star[4] = factor * (specific + (middle - speed) * (middle + pressure / mass))
    return [flux[c] + weight * (star[c] - state[c]) for c in range(6)]


def kernel(step_ref, low_ref, own_ref, high_ref, out_ref, signal_ref, prim, lower, upper, fluxes, gx):
    step = step_ref[0]
    half = 0.5 * step
    for source, start in ((low_ref, 0), (own_ref, 4), (high_ref, 8)):
        for layer in range(4):
            values = primitive_of([source[c, layer] for c in range(6)])
            for c in range(6):
                prim[c, start + layer] = values[c]

    def faces(index, carry):
        own = [prim[c, index + 3] for c in range(6)]
        edges = []
        for c in range(6):
            q = [prim[c, index + k] for k in range(7)]
            edges.append(
                limited(own[c], edge_of(*q[0:6]), edge_of(*q[1:7]))
            )
        for axis in range(3):
            if axis:
                edges = []
                for c in range(6):
                    q = own[c]
                    near = [roll(q, k, axis - 1) for k in (3, 2, 1)]
                    far = [roll(q, -k, axis - 1) for k in (1, 2)]
                    edge = edge_of(*near, q, *far)
                    edges.append(limited(q, edge, roll(edge, -1, axis - 1)))
            low_face, high_face = traced(own, edges, 1 + axis, half)
            for c in range(6):
                lower[axis, c, index] = low_face[c]
                upper[axis, c, index] = high_face[c]
        return carry

    lax.fori_loop(0, 6, faces, 0)

    def predicted(index, carry):
        for axis in (1, 2):
            left = [roll(upper[axis, c, index], 1, axis - 1) for c in range(6)]
            flux = hllc_flux(left, [lower[axis, c, index] for c in range(6)], 1 + axis)
            for c in range(6):
                fluxes[axis, c, index] = half * (roll(flux[c], -1, axis - 1) - flux[c])
        return carry

    lax.fori_loop(0, 6, predicted, 0)

    def predicted_first(index, carry):
        flux = hllc_flux(
            [upper[0, c, index] for c in range(6)], [lower[0, c, index + 1] for c in range(6)], 1
        )
        for c in range(6):
            fluxes[0, c, index] = flux[c]
        return carry

    lax.fori_loop(0, 5, predicted_first, 0)

    def corrected(states, changes):
        state = conserved_of(states)
        return primitive_of([state[c] - changes[c] for c in range(6)])

    def final_first(index, carry):
        change = [fluxes[1, c, index + 1, 0:8] + fluxes[2, c, index + 1, 0:8] for c in range(6)]
        before = [carry[c] for c in range(6)]
        right = corrected([lower[0, c, index + 1, 0:8] for c in range(6)], change)
        flux = hllc_flux(before, right, 1)
        for c in range(6):
            gx[c, index] = flux[c]
        return tuple(corrected([upper[0, c, index + 1, 0:8] for c in range(6)], change))

    change = [fluxes[1, c, 0, 0:8] + fluxes[2, c, 0, 0:8] for c in range(6)]
    first = tuple(corrected([upper[0, c, 0, 0:8] for c in range(6)], change))
    lax.fori_loop(0, 5, final_first, first)

    lanes = lax.broadcasted_iota(jnp.int32, (8, 128), 1) < 120

    def final(index, fastest):
        here = index + 1
        total = [own_ref[c, index, 0:8] - step * (gx[c, index + 1] - gx[c, index]) for c in range(6)]
        ahead = [half * (fluxes[0, c, here] - fluxes[0, c, index]) for c in range(6)]
        change = [ahead[c] + fluxes[2, c, here] for c in range(6)]
        left = corrected([upper[1, c, here] for c in range(6)], change)
        right = corrected([lower[1, c, here] for c in range(6)], change)
        flux = hllc_flux([roll(item, 1, 0) for item in left], right, 2)
        total = [total[c] - step * (roll(flux[c], -1, 0)[0:8] - flux[c][0:8]) for c in range(6)]
        change = [ahead[c][0:8] + fluxes[1, c, here, 0:8] for c in range(6)]
        left = corrected([upper[2, c, here, 0:8] for c in range(6)], change)
        right = corrected([lower[2, c, here, 0:8] for c in range(6)], change)
        flux = hllc_flux([roll(item, 1, 1) for item in left], right, 3)
        total = [total[c] - step * (roll(flux[c], -1, 1) - flux[c]) for c in range(6)]
        for c in range(6):
            out_ref[c, index] = total[c][:, 0:120]
        return jnp.maximum(fastest, jnp.where(lanes, fastest_signal(total), 0.0))

    fastest = lax.fori_loop(0, 4, final, jnp.zeros((8, 128), jnp.float32))
    signal_ref[0] = jnp.max(fastest)


def hydro_step(low, own, high, time_step):
    vmem = pl.BlockSpec(memory_space=pltpu.VMEM)
    smem = pl.BlockSpec(memory_space=pltpu.SMEM)
    return pl.pallas_call(
        kernel,
        in_specs=[smem, vmem, vmem, vmem],
        out_specs=[vmem, smem],
        out_shape=[
            jax.ShapeDtypeStruct((6, 4, 8, 120), jnp.float32),
            jax.ShapeDtypeStruct((1,), jnp.float32),
        ],
        scratch_shapes=[
            pltpu.VMEM((6, 12, 16, 128), jnp.float32),
            pltpu.VMEM((3, 6, 6, 16, 128), jnp.float32),
            pltpu.VMEM((3, 6, 6, 16, 128), jnp.float32),
            pltpu.VMEM((3, 6, 6, 16, 128), jnp.float32),
            pltpu.VMEM((6, 5, 8, 128), jnp.float32),
        ],
        name="hydro",
    )(time_step.reshape(1), low, own, high)


def step(conserved_state):
    signal_now = jnp.max(fastest_signal([conserved_state[component] for component in range(6)]))
    block = padded(conserved_state, GZ, lax.axis_index("y") % 2 == 1, 3, GHOST)
    signal_now = over_group(signal_now, PLANE)
    block = padded(block, GY, lax.axis_index("x") % 2 == 1, 2, GHOST)
    block, _ = lax.optimization_barrier((block, signal_now))
    signal_now = over_column(signal_now, 20)
    low, high = ghosts(block, GX, lax.axis_index("c") == 1, 1, GHOST)
    updated, signal_next = hydro_step(low, block, high, courant / signal_now)
    signal_next = over_group(signal_next[0], PLANE)
    signal_next = over_group(signal_next, COLUMN)
    return (updated, courant / signal_next)


def solution(mesh):
    finer = Mesh(mesh.devices.reshape(16, 2, 2, 4, 4), ALL)
    spec = P(None, GX, GY, GZ)
    return jax.shard_map(step, mesh=finer, in_specs=(spec,), out_specs=(spec, P()), check_vma=False)
```

```python
import jax
import jax.numpy as jnp
from jax import lax
from jax.experimental import pallas as pl
from jax.experimental.pallas import tpu as pltpu
from jax.sharding import Mesh
from jax.sharding import PartitionSpec as P

GHOST = 4
ALL = ("zl", "c", "zh", "x", "y")
PLANE = ("c", "x", "y")
COLUMN = ("zl", "zh")
GX = ("zl", "c")
GY = ("zh", "x")
GZ = ("y",)

adiabatic = 5.0 / 3.0
courant = 0.3


def over_group(value, axes):
    everyone = lax.all_to_all(
        jnp.broadcast_to(value, (lax.axis_size(axes),)), axes, 0, 0, tiled=True
    )
    return jnp.max(everyone)


def over_column(value, first):
    halves, rows = lax.axis_size("zh"), lax.axis_size("zl")
    deep = halves * rows
    order = [(first + step) % deep for step in range(deep)]
    columns, width = lax.axis_size("c"), lax.axis_size(("x", "y"))
    groups = [
        [(((z % rows) * columns + c) * halves + z // rows) * width + place for z in order]
        for c in range(columns)
        for place in range(width)
    ]
    everyone = lax.all_to_all(
        jnp.broadcast_to(value, (deep,)), ALL, 0, 0, axis_index_groups=groups, tiled=True
    )
    return jnp.max(everyone)


def swaps(count):
    even = [(i, i ^ 1) for i in range(count)]
    odd = [(i, (i + 1) % count if i % 2 else (i - 1) % count) for i in range(count)]
    return even, odd


def swapped(block, axes, parity, dim, width):
    even, odd = swaps(lax.axis_size(axes))
    first = lax.slice_in_dim(block, 0, width, axis=dim)
    last = lax.slice_in_dim(block, block.shape[dim] - width, None, axis=dim)
    if block.shape[dim] == width:
        to_even, to_odd = block, block
    else:
        to_even, to_odd = jnp.where(parity, first, last), jnp.where(parity, last, first)
    by_odd = lax.ppermute(to_odd, axes, odd)
    by_even = lax.ppermute(to_even, axes, even)
    return by_even, by_odd


def padded(block, axes, parity, dim, width):
    by_even, by_odd = swapped(block, axes, parity, dim, width)
    low, high = jnp.where(parity, by_even, by_odd), jnp.where(parity, by_odd, by_even)
    return jnp.concatenate([block, high, low], axis=dim)


def roll(value, shift, axis):
    return pltpu.roll(value, shift % value.shape[axis], axis)


def primitive_of(conserved):
    density, energy = conserved[0], conserved[4]
    inverse = 1.0 / density
    speed = [conserved[component] * inverse for component in (1, 2, 3)]
    kinetic = 0.5 * (conserved[1] * speed[0] + conserved[2] * speed[1] + conserved[3] * speed[2])
    return [density, *speed, (adiabatic - 1.0) * (energy - kinetic), conserved[5] * inverse]


def conserved_of(primitive):
    density = primitive[0]
    momenta = [density * primitive[component] for component in (1, 2, 3)]
    kinetic = 0.5 * (
        momenta[0] * primitive[1] + momenta[1] * primitive[2] + momenta[2] * primitive[3]
    )
    energy = primitive[4] * (1.0 / (adiabatic - 1.0)) + kinetic
    return [density, *momenta, energy, density * primitive[5]]


def fastest_signal(conserved):
    primitive = primitive_of(conserved)
    sound = jnp.sqrt(adiabatic * primitive[4] / primitive[0])
    speeds = jnp.maximum(
        jnp.maximum(jnp.abs(primitive[1]), jnp.abs(primitive[2])), jnp.abs(primitive[3])
    )
    return speeds + sound


def edge_of(q3, q2, q1, q, a1, a2):
    edge = (37.0 / 60.0) * (q1 + q) - (8.0 / 60.0) * (q2 + a1) + (1.0 / 60.0) * (q3 + a2)
    return jnp.clip(edge, jnp.minimum(q1, q), jnp.maximum(q1, q))


def limited(q, lower, upper):
    above, below = upper - q, q - lower
    spread = upper - lower
    skewed = spread * (0.5 * (below - above))
    limit = spread * spread * (1.0 / 6.0)
    flat = above * below <= 0.0
    new_lower = jnp.where(flat, q, jnp.where(skewed > limit, q - 2.0 * above, lower))
    new_upper = jnp.where(flat, q, jnp.where(skewed < -limit, q + 2.0 * below, upper))
    return new_lower, new_upper


def traced(primitive, edges, normal, half_step):
    slopes = [upper - lower for lower, upper in edges]
    density, speed, pressure = primitive[0], primitive[normal], primitive[4]
    rates = [-(speed * slopes[component]) for component in range(6)]
    rates[0] = rates[0] - density * slopes[normal]
    rates[normal] = rates[normal] - slopes[4] / density
    rates[4] = rates[4] - adiabatic * pressure * slopes[normal]
    moves = [half_step * rate for rate in rates]
    lower = [edges[component][0] + moves[component] for component in range(6)]
    upper = [edges[component][1] + moves[component] for component in range(6)]
    return lower, upper


def hllc_flux(left, right, normal):
    ratio_left, ratio_right = left[4] / left[0], right[4] / right[0]
    sound_left, sound_right = jnp.sqrt(adiabatic * ratio_left), jnp.sqrt(adiabatic * ratio_right)
    low = jnp.minimum(left[normal] - sound_left, right[normal] - sound_right)
    high = jnp.maximum(left[normal] + sound_left, right[normal] + sound_right)
    mass_left = left[0] * (low - left[normal])
    mass_right = right[0] * (high - right[normal])
    middle = (right[4] - left[4] + mass_left * left[normal] - mass_right * right[normal]) / (
        mass_left - mass_right
    )
    from_left = middle >= 0.0
    side = [jnp.where(from_left, left[component], right[component]) for component in range(6)]
    ratio = jnp.where(from_left, ratio_left, ratio_right)
    mass = jnp.where(from_left, mass_left, mass_right)
    outer = jnp.where(from_left, low, high)
    weight = jnp.where(from_left, jnp.minimum(low, 0.0), jnp.maximum(high, 0.0))
    speed, pressure = side[normal], side[4]
    state = conserved_of(side)
    flux = [item * speed for item in state]
    flux[normal] = flux[normal] + pressure
    flux[4] = flux[4] + pressure * speed
    factor = mass / (outer - middle)
    star = [factor * item for item in side]
    star[0] = factor
    star[normal] = factor * middle
    half_square = 0.5 * (side[1] * side[1] + side[2] * side[2] + side[3] * side[3])
    specific = ratio * (1.0 / (adiabatic - 1.0)) + half_square
    star[4] = factor * (specific + (middle - speed) * (middle + pressure / mass))
    return [flux[c] + weight * (star[c] - state[c]) for c in range(6)]


def kernel(parity_ref, step_ref, even_ref, own_ref, odd_ref, out_ref, signal_ref, prim, lower, upper, fluxes, gx):
    step = step_ref[0]
    half = 0.5 * step
    even_start = 8 - 8 * parity_ref[0]
    for source, start in ((even_ref, even_start), (own_ref, 4), (odd_ref, 8 - even_start)):
        for layer in range(4):
            values = primitive_of([source[c, layer] for c in range(6)])
            for c in range(6):
                prim[c, start + layer] = values[c]

    def faces(index, carry):
        own = [prim[c, index + 3] for c in range(6)]
        edges = []
        for c in range(6):
            q = [prim[c, index + k] for k in range(7)]
            edges.append(
                limited(own[c], edge_of(*q[0:6]), edge_of(*q[1:7]))
            )
        for axis in range(3):
            if axis:
                edges = []
                for c in range(6):
                    q = own[c]
                    near = [roll(q, k, axis - 1) for k in (3, 2, 1)]
                    far = [roll(q, -k, axis - 1) for k in (1, 2)]
                    edge = edge_of(*near, q, *far)
                    edges.append(limited(q, edge, roll(edge, -1, axis - 1)))
            low_face, high_face = traced(own, edges, 1 + axis, half)
            for c in range(6):
                lower[axis, c, index] = low_face[c]
                upper[axis, c, index] = high_face[c]
        return carry

    lax.fori_loop(0, 6, faces, 0)

    def predicted(index, carry):
        for axis in (1, 2):
            left = [roll(upper[axis, c, index], 1, axis - 1) for c in range(6)]
            flux = hllc_flux(left, [lower[axis, c, index] for c in range(6)], 1 + axis)
            for c in range(6):
                fluxes[axis, c, index] = half * (roll(flux[c], -1, axis - 1) - flux[c])
        return carry

    lax.fori_loop(0, 6, predicted, 0)

    def predicted_first(index, carry):
        flux = hllc_flux(
            [upper[0, c, index] for c in range(6)], [lower[0, c, index + 1] for c in range(6)], 1
        )
        for c in range(6):
            fluxes[0, c, index] = flux[c]
        return carry

    lax.fori_loop(0, 5, predicted_first, 0)

    def corrected(states, changes):
        state = conserved_of(states)
        return primitive_of([state[c] - changes[c] for c in range(6)])

    def final_first(index, carry):
        change = [fluxes[1, c, index + 1, 0:8] + fluxes[2, c, index + 1, 0:8] for c in range(6)]
        before = [carry[c] for c in range(6)]
        right = corrected([lower[0, c, index + 1, 0:8] for c in range(6)], change)
        flux = hllc_flux(before, right, 1)
        for c in range(6):
            gx[c, index] = flux[c]
        return tuple(corrected([upper[0, c, index + 1, 0:8] for c in range(6)], change))

    change = [fluxes[1, c, 0, 0:8] + fluxes[2, c, 0, 0:8] for c in range(6)]
    first = tuple(corrected([upper[0, c, 0, 0:8] for c in range(6)], change))
    lax.fori_loop(0, 5, final_first, first)

    lanes = lax.broadcasted_iota(jnp.int32, (8, 128), 1) < 120

    def final(index, fastest):
        here = index + 1
        total = [own_ref[c, index, 0:8] - step * (gx[c, index + 1] - gx[c, index]) for c in range(6)]
        ahead = [half * (fluxes[0, c, here] - fluxes[0, c, index]) for c in range(6)]
        change = [ahead[c] + fluxes[2, c, here] for c in range(6)]
        left = corrected([upper[1, c, here] for c in range(6)], change)
        right = corrected([lower[1, c, here] for c in range(6)], change)
        flux = hllc_flux([roll(item, 1, 0) for item in left], right, 2)
        total = [total[c] - step * (roll(flux[c], -1, 0)[0:8] - flux[c][0:8]) for c in range(6)]
        change = [ahead[c][0:8] + fluxes[1, c, here, 0:8] for c in range(6)]
        left = corrected([upper[2, c, here, 0:8] for c in range(6)], change)
        right = corrected([lower[2, c, here, 0:8] for c in range(6)], change)
        flux = hllc_flux([roll(item, 1, 1) for item in left], right, 3)
        total = [total[c] - step * (roll(flux[c], -1, 1) - flux[c]) for c in range(6)]
        for c in range(6):
            out_ref[c, index] = total[c][:, 0:120]
        return jnp.maximum(fastest, jnp.where(lanes, fastest_signal(total), 0.0))

    fastest = lax.fori_loop(0, 4, final, jnp.zeros((8, 128), jnp.float32))
    signal_ref[0] = jnp.max(fastest)


def hydro_step(parity, time_step, by_even, own, by_odd):
    vmem = pl.BlockSpec(memory_space=pltpu.VMEM)
    smem = pl.BlockSpec(memory_space=pltpu.SMEM)
    blocks = [pltpu.with_memory_space_constraint(item, pltpu.VMEM) for item in (by_even, own, by_odd)]
    return pl.pallas_call(
        kernel,
        in_specs=[smem, smem, vmem, vmem, vmem],
        out_specs=[vmem, smem],
        out_shape=[
            jax.ShapeDtypeStruct((6, 4, 8, 120), jnp.float32),
            jax.ShapeDtypeStruct((1,), jnp.float32),
        ],
        scratch_shapes=[
            pltpu.VMEM((6, 12, 16, 128), jnp.float32),
            pltpu.VMEM((3, 6, 6, 16, 128), jnp.float32),
            pltpu.VMEM((3, 6, 6, 16, 128), jnp.float32),
            pltpu.VMEM((3, 6, 6, 16, 128), jnp.float32),
            pltpu.VMEM((6, 5, 8, 128), jnp.float32),
        ],
        name="hydro",
    )(parity.reshape(1), time_step.reshape(1), *blocks)


def step(conserved_state):
    signal_now = jnp.max(fastest_signal([conserved_state[component] for component in range(6)]))
    block = padded(conserved_state, GZ, lax.axis_index("y") % 2 == 1, 3, GHOST)
    to_plane = jnp.broadcast_to(signal_now, (lax.axis_size(PLANE), 1, 1))
    block, to_plane = lax.optimization_barrier((block, to_plane))
    signal_now = jnp.max(lax.all_to_all(to_plane, PLANE, 0, 0, tiled=True))
    block = padded(block, GY, lax.axis_index("x") % 2 == 1, 2, GHOST)
    block, _ = lax.optimization_barrier((block, signal_now))
    signal_now = over_column(signal_now, 8)
    parity = lax.axis_index("c")
    by_even, by_odd = swapped(block, GX, parity == 1, 1, GHOST)
    updated, signal_next = hydro_step(parity, courant / signal_now, by_even, block, by_odd)
    signal_next = over_group(signal_next[0], PLANE)
    signal_next = over_group(signal_next, COLUMN)
    return (updated, courant / signal_next)


def solution(mesh):
    finer = Mesh(mesh.devices.reshape(16, 2, 2, 4, 4), ALL)
    spec = P(None, GX, GY, GZ)
    return jax.shard_map(step, mesh=finer, in_specs=(spec,), out_specs=(spec, P()), check_vma=False)
```

```python
import jax
import jax.numpy as jnp
from jax import lax
from jax.experimental import pallas as pl
from jax.experimental.pallas import tpu as pltpu
from jax.sharding import Mesh
from jax.sharding import PartitionSpec as P

GHOST = 4
ALL = ("zl", "c", "zh", "x", "y")
PLANE = ("c", "x", "y")
COLUMN = ("zl", "zh")
GX = ("zl", "c")
GY = ("zh", "x")
GZ = ("y",)

adiabatic = 5.0 / 3.0
courant = 0.3


def over_column(value, first):
    halves, rows = lax.axis_size("zh"), lax.axis_size("zl")
    deep = halves * rows
    order = [(first + step) % deep for step in range(deep)]
    columns, width = lax.axis_size("c"), lax.axis_size(("x", "y"))
    groups = [
        [(((z % rows) * columns + c) * halves + z // rows) * width + place for z in order]
        for c in range(columns)
        for place in range(width)
    ]
    value = jnp.broadcast_to(value, (deep, 1, 1))
    return lax.all_to_all(value, ALL, 0, 0, axis_index_groups=groups, tiled=True)


def swaps(count):
    even = [(i, i ^ 1) for i in range(count)]
    odd = [(i, (i + 1) % count if i % 2 else (i - 1) % count) for i in range(count)]
    return even, odd


def swapped(block, axes, parity, dim, width):
    even, odd = swaps(lax.axis_size(axes))
    first = lax.slice_in_dim(block, 0, width, axis=dim)
    last = lax.slice_in_dim(block, block.shape[dim] - width, None, axis=dim)
    if block.shape[dim] == width:
        to_even, to_odd = block, block
    else:
        to_even, to_odd = jnp.where(parity, first, last), jnp.where(parity, last, first)
    by_odd = lax.ppermute(to_odd, axes, odd)
    by_even = lax.ppermute(to_even, axes, even)
    return by_even, by_odd


def padded(block, axes, parity, dim, width):
    by_even, by_odd = swapped(block, axes, parity, dim, width)
    low, high = jnp.where(parity, by_even, by_odd), jnp.where(parity, by_odd, by_even)
    return jnp.concatenate([block, high, low], axis=dim)


def roll(value, shift, axis):
    return pltpu.roll(value, shift % value.shape[axis], axis)


def primitive_of(conserved):
    density, energy = conserved[0], conserved[4]
    inverse = 1.0 / density
    speed = [conserved[component] * inverse for component in (1, 2, 3)]
    kinetic = 0.5 * (conserved[1] * speed[0] + conserved[2] * speed[1] + conserved[3] * speed[2])
    return [density, *speed, (adiabatic - 1.0) * (energy - kinetic), conserved[5] * inverse]


def conserved_of(primitive):
    density = primitive[0]
    momenta = [density * primitive[component] for component in (1, 2, 3)]
    kinetic = 0.5 * (
        momenta[0] * primitive[1] + momenta[1] * primitive[2] + momenta[2] * primitive[3]
    )
    energy = primitive[4] * (1.0 / (adiabatic - 1.0)) + kinetic
    return [density, *momenta, energy, density * primitive[5]]


def fastest_signal(conserved):
    primitive = primitive_of(conserved)
    sound = jnp.sqrt(adiabatic * primitive[4] / primitive[0])
    speeds = jnp.maximum(
        jnp.maximum(jnp.abs(primitive[1]), jnp.abs(primitive[2])), jnp.abs(primitive[3])
    )
    return speeds + sound


def edge_of(q3, q2, q1, q, a1, a2):
    edge = (37.0 / 60.0) * (q1 + q) - (8.0 / 60.0) * (q2 + a1) + (1.0 / 60.0) * (q3 + a2)
    return jnp.clip(edge, jnp.minimum(q1, q), jnp.maximum(q1, q))


def limited(q, lower, upper):
    above, below = upper - q, q - lower
    spread = upper - lower
    skewed = spread * (0.5 * (below - above))
    limit = spread * spread * (1.0 / 6.0)
    flat = above * below <= 0.0
    new_lower = jnp.where(flat, q, jnp.where(skewed > limit, q - 2.0 * above, lower))
    new_upper = jnp.where(flat, q, jnp.where(skewed < -limit, q + 2.0 * below, upper))
    return new_lower, new_upper


def traced(primitive, edges, normal, half_step):
    slopes = [upper - lower for lower, upper in edges]
    density, speed, pressure = primitive[0], primitive[normal], primitive[4]
    rates = [-(speed * slopes[component]) for component in range(6)]
    rates[0] = rates[0] - density * slopes[normal]
    rates[normal] = rates[normal] - slopes[4] / density
    rates[4] = rates[4] - adiabatic * pressure * slopes[normal]
    moves = [half_step * rate for rate in rates]
    lower = [edges[component][0] + moves[component] for component in range(6)]
    upper = [edges[component][1] + moves[component] for component in range(6)]
    return lower, upper


def hllc_flux(left, right, normal):
    ratio_left, ratio_right = left[4] / left[0], right[4] / right[0]
    sound_left, sound_right = jnp.sqrt(adiabatic * ratio_left), jnp.sqrt(adiabatic * ratio_right)
    low = jnp.minimum(left[normal] - sound_left, right[normal] - sound_right)
    high = jnp.maximum(left[normal] + sound_left, right[normal] + sound_right)
    mass_left = left[0] * (low - left[normal])
    mass_right = right[0] * (high - right[normal])
    middle = (right[4] - left[4] + mass_left * left[normal] - mass_right * right[normal]) / (
        mass_left - mass_right
    )
    from_left = middle >= 0.0
    side = [jnp.where(from_left, left[component], right[component]) for component in range(6)]
    ratio = jnp.where(from_left, ratio_left, ratio_right)
    mass = jnp.where(from_left, mass_left, mass_right)
    outer = jnp.where(from_left, low, high)
    weight = jnp.where(from_left, jnp.minimum(low, 0.0), jnp.maximum(high, 0.0))
    speed, pressure = side[normal], side[4]
    state = conserved_of(side)
    flux = [item * speed for item in state]
    flux[normal] = flux[normal] + pressure
    flux[4] = flux[4] + pressure * speed
    factor = mass / (outer - middle)
    star = [factor * item for item in side]
    star[0] = factor
    star[normal] = factor * middle
    half_square = 0.5 * (side[1] * side[1] + side[2] * side[2] + side[3] * side[3])
    specific = ratio * (1.0 / (adiabatic - 1.0)) + half_square
    star[4] = factor * (specific + (middle - speed) * (middle + pressure / mass))
    return [flux[c] + weight * (star[c] - state[c]) for c in range(6)]


def maximum_of(everyone_ref):
    fastest = everyone_ref[0]
    for device in range(1, everyone_ref.shape[0]):
        fastest = jnp.maximum(fastest, everyone_ref[device])
    return fastest


def spread_kernel(everyone_ref, out_ref):
    out_ref[...] = jnp.broadcast_to(maximum_of(everyone_ref)[None], out_ref.shape)


def spread(everyone, count):
    vmem = pl.BlockSpec(memory_space=pltpu.VMEM)
    return pl.pallas_call(
        spread_kernel,
        in_specs=[vmem],
        out_specs=vmem,
        out_shape=jax.ShapeDtypeStruct((count, 1, 1), jnp.float32),
        name="spread",
    )(pltpu.with_memory_space_constraint(everyone, pltpu.VMEM))


def kernel(column_ref, even_ref, own_ref, odd_ref, out_ref, signal_ref, prim, lower, upper, fluxes, gx):
    step = jnp.max(courant / maximum_of(column_ref))
    half = 0.5 * step
    even_start = 8 - 8 * lax.axis_index("c")
    for source, start in ((even_ref, even_start), (own_ref, 4), (odd_ref, 8 - even_start)):
        for layer in range(4):
            values = primitive_of([source[c, layer] for c in range(6)])
            for c in range(6):
                prim[c, start + layer] = values[c]

    def faces(index, carry):
        own = [prim[c, index + 3] for c in range(6)]
        edges = []
        for c in range(6):
            q = [prim[c, index + k] for k in range(7)]
            edges.append(
                limited(own[c], edge_of(*q[0:6]), edge_of(*q[1:7]))
            )
        for axis in range(3):
            if axis:
                edges = []
                for c in range(6):
                    q = own[c]
                    near = [roll(q, k, axis - 1) for k in (3, 2, 1)]
                    far = [roll(q, -k, axis - 1) for k in (1, 2)]
                    edge = edge_of(*near, q, *far)
                    edges.append(limited(q, edge, roll(edge, -1, axis - 1)))
            low_face, high_face = traced(own, edges, 1 + axis, half)
            for c in range(6):
                lower[axis, c, index] = low_face[c]
                upper[axis, c, index] = high_face[c]
        return carry

    lax.fori_loop(0, 6, faces, 0)

    def predicted(index, carry):
        for axis in (1, 2):
            left = [roll(upper[axis, c, index], 1, axis - 1) for c in range(6)]
            flux = hllc_flux(left, [lower[axis, c, index] for c in range(6)], 1 + axis)
            for c in range(6):
                fluxes[axis, c, index] = half * (roll(flux[c], -1, axis - 1) - flux[c])
        return carry

    lax.fori_loop(0, 6, predicted, 0)

    def predicted_first(index, carry):
        flux = hllc_flux(
            [upper[0, c, index] for c in range(6)], [lower[0, c, index + 1] for c in range(6)], 1
        )
        for c in range(6):
            fluxes[0, c, index] = flux[c]
        return carry

    lax.fori_loop(0, 5, predicted_first, 0)

    def corrected(states, changes):
        state = conserved_of(states)
        return primitive_of([state[c] - changes[c] for c in range(6)])

    def final_first(index, carry):
        change = [fluxes[1, c, index + 1, 0:8] + fluxes[2, c, index + 1, 0:8] for c in range(6)]
        before = [carry[c] for c in range(6)]
        right = corrected([lower[0, c, index + 1, 0:8] for c in range(6)], change)
        flux = hllc_flux(before, right, 1)
        for c in range(6):
            gx[c, index] = flux[c]
        return tuple(corrected([upper[0, c, index + 1, 0:8] for c in range(6)], change))

    change = [fluxes[1, c, 0, 0:8] + fluxes[2, c, 0, 0:8] for c in range(6)]
    first = tuple(corrected([upper[0, c, 0, 0:8] for c in range(6)], change))
    lax.fori_loop(0, 5, final_first, first)

    lanes = lax.broadcasted_iota(jnp.int32, (8, 128), 1) < 120

    def final(index, fastest):
        here = index + 1
        total = [own_ref[c, index, 0:8] - step * (gx[c, index + 1] - gx[c, index]) for c in range(6)]
        ahead = [half * (fluxes[0, c, here] - fluxes[0, c, index]) for c in range(6)]
        change = [ahead[c] + fluxes[2, c, here] for c in range(6)]
        left = corrected([upper[1, c, here] for c in range(6)], change)
        right = corrected([lower[1, c, here] for c in range(6)], change)
        flux = hllc_flux([roll(item, 1, 0) for item in left], right, 2)
        total = [total[c] - step * (roll(flux[c], -1, 0)[0:8] - flux[c][0:8]) for c in range(6)]
        change = [ahead[c][0:8] + fluxes[1, c, here, 0:8] for c in range(6)]
        left = corrected([upper[2, c, here, 0:8] for c in range(6)], change)
        right = corrected([lower[2, c, here, 0:8] for c in range(6)], change)
        flux = hllc_flux([roll(item, 1, 1) for item in left], right, 3)
        total = [total[c] - step * (roll(flux[c], -1, 1) - flux[c]) for c in range(6)]
        for c in range(6):
            out_ref[c, index] = total[c][:, 0:120]
        return jnp.maximum(fastest, jnp.where(lanes, fastest_signal(total), 0.0))

    fastest = lax.fori_loop(0, 4, final, jnp.zeros((8, 128), jnp.float32))
    signal_ref[...] = jnp.full(signal_ref.shape, jnp.max(fastest))


def hydro_step(column, by_even, own, by_odd, count):
    vmem = pl.BlockSpec(memory_space=pltpu.VMEM)
    blocks = [
        pltpu.with_memory_space_constraint(item, pltpu.VMEM)
        for item in (column, by_even, own, by_odd)
    ]
    return pl.pallas_call(
        kernel,
        in_specs=[vmem] * 4,
        out_specs=[vmem, vmem],
        out_shape=[
            jax.ShapeDtypeStruct((6, 4, 8, 120), jnp.float32),
            jax.ShapeDtypeStruct((count, 1, 1), jnp.float32),
        ],
        scratch_shapes=[
            pltpu.VMEM((6, 12, 16, 128), jnp.float32),
            pltpu.VMEM((3, 6, 6, 16, 128), jnp.float32),
            pltpu.VMEM((3, 6, 6, 16, 128), jnp.float32),
            pltpu.VMEM((3, 6, 6, 16, 128), jnp.float32),
            pltpu.VMEM((6, 5, 8, 128), jnp.float32),
        ],
        name="hydro",
    )(*blocks)


def step(conserved_state):
    signal_now = jnp.max(fastest_signal([conserved_state[component] for component in range(6)]))
    block = padded(conserved_state, GZ, lax.axis_index("y") % 2 == 1, 3, GHOST)
    to_plane = jnp.broadcast_to(signal_now, (lax.axis_size(PLANE), 1, 1))
    block, to_plane = lax.optimization_barrier((block, to_plane))
    signal_now = jnp.max(lax.all_to_all(to_plane, PLANE, 0, 0, tiled=True))
    block = padded(block, GY, lax.axis_index("x") % 2 == 1, 2, GHOST)
    block, _ = lax.optimization_barrier((block, signal_now))
    column = over_column(signal_now, 8)
    by_even, by_odd = swapped(block, GX, lax.axis_index("c") == 1, 1, GHOST)
    updated, to_plane = hydro_step(column, by_even, block, by_odd, lax.axis_size(PLANE))
    plane = lax.all_to_all(to_plane, PLANE, 0, 0, tiled=True)
    to_column = spread(plane, lax.axis_size(COLUMN))
    column = lax.all_to_all(to_column, COLUMN, 0, 0, tiled=True)
    return (updated, courant / jnp.max(column))


def solution(mesh):
    finer = Mesh(mesh.devices.reshape(16, 2, 2, 4, 4), ALL)
    spec = P(None, GX, GY, GZ)
    return jax.shard_map(step, mesh=finer, in_specs=(spec,), out_specs=(spec, P()), check_vma=False)
```

```python
import jax
import jax.numpy as jnp
from jax import lax
from jax.experimental import pallas as pl
from jax.experimental.pallas import tpu as pltpu
from jax.sharding import Mesh
from jax.sharding import PartitionSpec as P

GHOST = 4
ALL = ("zl", "c", "zh", "x", "y")
PLANE = ("c", "x", "y")
COLUMN = ("zl", "zh")
GX = ("zl", "c")
GY = ("zh", "x")
GZ = ("y",)

adiabatic = 5.0 / 3.0
courant = 0.3


def over_column(value, first):
    halves, rows = lax.axis_size("zh"), lax.axis_size("zl")
    deep = halves * rows
    order = [(first + step) % deep for step in range(deep)]
    columns, width = lax.axis_size("c"), lax.axis_size(("x", "y"))
    groups = [
        [(((z % rows) * columns + c) * halves + z // rows) * width + place for z in order]
        for c in range(columns)
        for place in range(width)
    ]
    return lax.all_to_all(value, ALL, 0, 0, axis_index_groups=groups, tiled=True)


def swaps(count):
    even = [(i, i ^ 1) for i in range(count)]
    odd = [(i, (i + 1) % count if i % 2 else (i - 1) % count) for i in range(count)]
    return even, odd


def swapped(block, axes, parity, dim, width):
    even, odd = swaps(lax.axis_size(axes))
    first = lax.slice_in_dim(block, 0, width, axis=dim)
    last = lax.slice_in_dim(block, block.shape[dim] - width, None, axis=dim)
    if block.shape[dim] == width:
        to_even, to_odd = block, block
    else:
        to_even, to_odd = jnp.where(parity, first, last), jnp.where(parity, last, first)
    by_odd = lax.ppermute(to_odd, axes, odd)
    by_even = lax.ppermute(to_even, axes, even)
    return by_even, by_odd


def padded(block, axes, parity, dim, width):
    by_even, by_odd = swapped(block, axes, parity, dim, width)
    low, high = jnp.where(parity, by_even, by_odd), jnp.where(parity, by_odd, by_even)
    return jnp.concatenate([block, high, low], axis=dim)


def roll(value, shift, axis):
    return pltpu.roll(value, shift % value.shape[axis], axis)


def primitive_of(conserved):
    density, energy = conserved[0], conserved[4]
    inverse = 1.0 / density
    speed = [conserved[component] * inverse for component in (1, 2, 3)]
    kinetic = 0.5 * (conserved[1] * speed[0] + conserved[2] * speed[1] + conserved[3] * speed[2])
    return [density, *speed, (adiabatic - 1.0) * (energy - kinetic), conserved[5] * inverse]


def conserved_of(primitive):
    density = primitive[0]
    momenta = [density * primitive[component] for component in (1, 2, 3)]
    kinetic = 0.5 * (
        momenta[0] * primitive[1] + momenta[1] * primitive[2] + momenta[2] * primitive[3]
    )
    energy = primitive[4] * (1.0 / (adiabatic - 1.0)) + kinetic
    return [density, *momenta, energy, density * primitive[5]]


def fastest_signal(conserved):
    primitive = primitive_of(conserved)
    sound = jnp.sqrt(adiabatic * primitive[4] / primitive[0])
    speeds = jnp.maximum(
        jnp.maximum(jnp.abs(primitive[1]), jnp.abs(primitive[2])), jnp.abs(primitive[3])
    )
    return speeds + sound


def edge_of(q3, q2, q1, q, a1, a2):
    edge = (37.0 / 60.0) * (q1 + q) - (8.0 / 60.0) * (q2 + a1) + (1.0 / 60.0) * (q3 + a2)
    return jnp.clip(edge, jnp.minimum(q1, q), jnp.maximum(q1, q))


def limited(q, lower, upper):
    above, below = upper - q, q - lower
    spread = upper - lower
    skewed = spread * (0.5 * (below - above))
    limit = spread * spread * (1.0 / 6.0)
    flat = above * below <= 0.0
    new_lower = jnp.where(flat, q, jnp.where(skewed > limit, q - 2.0 * above, lower))
    new_upper = jnp.where(flat, q, jnp.where(skewed < -limit, q + 2.0 * below, upper))
    return new_lower, new_upper


def traced(primitive, edges, normal, half_step):
    slopes = [upper - lower for lower, upper in edges]
    density, speed, pressure = primitive[0], primitive[normal], primitive[4]
    rates = [-(speed * slopes[component]) for component in range(6)]
    rates[0] = rates[0] - density * slopes[normal]
    rates[normal] = rates[normal] - slopes[4] / density
    rates[4] = rates[4] - adiabatic * pressure * slopes[normal]
    moves = [half_step * rate for rate in rates]
    lower = [edges[component][0] + moves[component] for component in range(6)]
    upper = [edges[component][1] + moves[component] for component in range(6)]
    return lower, upper


def hllc_flux(left, right, normal):
    ratio_left, ratio_right = left[4] / left[0], right[4] / right[0]
    sound_left, sound_right = jnp.sqrt(adiabatic * ratio_left), jnp.sqrt(adiabatic * ratio_right)
    low = jnp.minimum(left[normal] - sound_left, right[normal] - sound_right)
    high = jnp.maximum(left[normal] + sound_left, right[normal] + sound_right)
    mass_left = left[0] * (low - left[normal])
    mass_right = right[0] * (high - right[normal])
    middle = (right[4] - left[4] + mass_left * left[normal] - mass_right * right[normal]) / (
        mass_left - mass_right
    )
    from_left = middle >= 0.0
    side = [jnp.where(from_left, left[component], right[component]) for component in range(6)]
    ratio = jnp.where(from_left, ratio_left, ratio_right)
    mass = jnp.where(from_left, mass_left, mass_right)
    outer = jnp.where(from_left, low, high)
    weight = jnp.where(from_left, jnp.minimum(low, 0.0), jnp.maximum(high, 0.0))
    speed, pressure = side[normal], side[4]
    state = conserved_of(side)
    flux = [item * speed for item in state]
    flux[normal] = flux[normal] + pressure
    flux[4] = flux[4] + pressure * speed
    factor = mass / (outer - middle)
    star = [factor * item for item in side]
    star[0] = factor
    star[normal] = factor * middle
    half_square = 0.5 * (side[1] * side[1] + side[2] * side[2] + side[3] * side[3])
    specific = ratio * (1.0 / (adiabatic - 1.0)) + half_square
    star[4] = factor * (specific + (middle - speed) * (middle + pressure / mass))
    return [flux[c] + weight * (star[c] - state[c]) for c in range(6)]


def maximum_of(everyone_ref):
    fastest = everyone_ref[0]
    for device in range(1, everyone_ref.shape[0]):
        fastest = jnp.maximum(fastest, everyone_ref[device])
    return fastest


def spread_kernel(everyone_ref, out_ref):
    out_ref[...] = jnp.broadcast_to(maximum_of(everyone_ref)[None], out_ref.shape)


def spread(everyone, count):
    vmem = pl.BlockSpec(memory_space=pltpu.VMEM)
    return pl.pallas_call(
        spread_kernel,
        in_specs=[vmem],
        out_specs=vmem,
        out_shape=jax.ShapeDtypeStruct((count, 1, 1), jnp.float32),
        name="spread",
    )(pltpu.with_memory_space_constraint(everyone, pltpu.VMEM))


def lane_ids():
    return lax.broadcasted_iota(jnp.int32, (8, 128), 1)


def pack_kernel(state_ref, out_ref, wide):
    lanes = lane_ids()
    for c in range(6):
        for layer in range(4):
            wide[c, layer, :, 0:120] = state_ref[c, layer]
    fastest = jnp.zeros((8, 128), jnp.float32)
    for layer in range(4):
        signal = fastest_signal([wide[c, layer] for c in range(6)])
        fastest = jnp.maximum(fastest, jnp.where(lanes < 120, signal, 0.0))
    first = last = jnp.full((8, 128), jnp.max(fastest))
    for c in range(6):
        for layer in range(4):
            spot = 4 * (4 * c + layer)
            here = (lanes >= spot) & (lanes < spot + 4)
            first = jnp.where(here, roll(wide[c, layer], spot, 1), first)
            last = jnp.where(here, roll(wide[c, layer], spot - 116, 1), last)
    above = lax.rem(lax.axis_index("y") + 1, 4)
    for y in range(4):
        tile = jnp.where(above == y, last, first)
        for place in range(y, 32, 4):
            out_ref[place] = tile


def unpack_kernel(state_ref, tiles_ref, block_ref, column_ref):
    lanes = lane_ids()
    fastest = tiles_ref[0]
    for place in range(1, 32):
        fastest = jnp.maximum(fastest, tiles_ref[place])
    fastest = jnp.max(jnp.where(lanes >= 96, fastest, 0.0))
    column_ref[...] = jnp.full(column_ref.shape, fastest)
    y = lax.axis_index("y")
    base = 16 * lax.axis_index("c") + 4 * lax.axis_index("x")
    below = tiles_ref[base + lax.rem(y + 3, 4)]
    above = tiles_ref[base + lax.rem(y + 1, 4)]
    for c in range(6):
        for layer in range(4):
            spot = 4 * (4 * c + layer)
            ghosts = jnp.where(lanes < 124, roll(above, 120 - spot, 1), roll(below, 124 - spot, 1))
            block_ref[c, layer] = ghosts
            block_ref[c, layer, :, 0:120] = state_ref[c, layer]


def in_vmem(*arrays):
    return [pltpu.with_memory_space_constraint(item, pltpu.VMEM) for item in arrays]


def packed(state):
    vmem = pl.BlockSpec(memory_space=pltpu.VMEM)
    return pl.pallas_call(
        pack_kernel,
        in_specs=[vmem],
        out_specs=vmem,
        out_shape=jax.ShapeDtypeStruct((32, 8, 128), jnp.float32),
        scratch_shapes=[pltpu.VMEM((6, 4, 8, 128), jnp.float32)],
        name="pack",
    )(*in_vmem(state))


def unpacked(state, tiles, count):
    vmem = pl.BlockSpec(memory_space=pltpu.VMEM)
    return pl.pallas_call(
        unpack_kernel,
        in_specs=[vmem, vmem],
        out_specs=[vmem, vmem],
        out_shape=[
            jax.ShapeDtypeStruct((6, 4, 8, 128), jnp.float32),
            jax.ShapeDtypeStruct((count, 1, 1), jnp.float32),
        ],
        name="unpack",
    )(*in_vmem(state, tiles))


def kernel(column_ref, even_ref, own_ref, odd_ref, out_ref, signal_ref, prim, lower, upper, fluxes, gx):
    step = jnp.max(courant / maximum_of(column_ref))
    half = 0.5 * step
    even_start = 8 - 8 * lax.axis_index("c")
    for source, start in ((even_ref, even_start), (own_ref, 4), (odd_ref, 8 - even_start)):
        for layer in range(4):
            values = primitive_of([source[c, layer] for c in range(6)])
            for c in range(6):
                prim[c, start + layer] = values[c]

    def faces(index, carry):
        own = [prim[c, index + 3] for c in range(6)]
        edges = []
        for c in range(6):
            q = [prim[c, index + k] for k in range(7)]
            edges.append(
                limited(own[c], edge_of(*q[0:6]), edge_of(*q[1:7]))
            )
        for axis in range(3):
            if axis:
                edges = []
                for c in range(6):
                    q = own[c]
                    near = [roll(q, k, axis - 1) for k in (3, 2, 1)]
                    far = [roll(q, -k, axis - 1) for k in (1, 2)]
                    edge = edge_of(*near, q, *far)
                    edges.append(limited(q, edge, roll(edge, -1, axis - 1)))
            low_face, high_face = traced(own, edges, 1 + axis, half)
            for c in range(6):
                lower[axis, c, index] = low_face[c]
                upper[axis, c, index] = high_face[c]
        return carry

    lax.fori_loop(0, 6, faces, 0)

    def predicted(index, carry):
        for axis in (1, 2):
            left = [roll(upper[axis, c, index], 1, axis - 1) for c in range(6)]
            flux = hllc_flux(left, [lower[axis, c, index] for c in range(6)], 1 + axis)
            for c in range(6):
                fluxes[axis, c, index] = half * (roll(flux[c], -1, axis - 1) - flux[c])
        return carry

    lax.fori_loop(0, 6, predicted, 0)

    def predicted_first(index, carry):
        flux = hllc_flux(
            [upper[0, c, index] for c in range(6)], [lower[0, c, index + 1] for c in range(6)], 1
        )
        for c in range(6):
            fluxes[0, c, index] = flux[c]
        return carry

    lax.fori_loop(0, 5, predicted_first, 0)

    def corrected(states, changes):
        state = conserved_of(states)
        return primitive_of([state[c] - changes[c] for c in range(6)])

    def final_first(index, carry):
        change = [fluxes[1, c, index + 1, 0:8] + fluxes[2, c, index + 1, 0:8] for c in range(6)]
        before = [carry[c] for c in range(6)]
        right = corrected([lower[0, c, index + 1, 0:8] for c in range(6)], change)
        flux = hllc_flux(before, right, 1)
        for c in range(6):
            gx[c, index] = flux[c]
        return tuple(corrected([upper[0, c, index + 1, 0:8] for c in range(6)], change))

    change = [fluxes[1, c, 0, 0:8] + fluxes[2, c, 0, 0:8] for c in range(6)]
    first = tuple(corrected([upper[0, c, 0, 0:8] for c in range(6)], change))
    lax.fori_loop(0, 5, final_first, first)

    lanes = lane_ids() < 120

    def final(index, fastest):
        here = index + 1
        total = [own_ref[c, index, 0:8] - step * (gx[c, index + 1] - gx[c, index]) for c in range(6)]
        ahead = [half * (fluxes[0, c, here] - fluxes[0, c, index]) for c in range(6)]
        change = [ahead[c] + fluxes[2, c, here] for c in range(6)]
        left = corrected([upper[1, c, here] for c in range(6)], change)
        right = corrected([lower[1, c, here] for c in range(6)], change)
        flux = hllc_flux([roll(item, 1, 0) for item in left], right, 2)
        total = [total[c] - step * (roll(flux[c], -1, 0)[0:8] - flux[c][0:8]) for c in range(6)]
        change = [ahead[c][0:8] + fluxes[1, c, here, 0:8] for c in range(6)]
        left = corrected([upper[2, c, here, 0:8] for c in range(6)], change)
        right = corrected([lower[2, c, here, 0:8] for c in range(6)], change)
        flux = hllc_flux([roll(item, 1, 1) for item in left], right, 3)
        total = [total[c] - step * (roll(flux[c], -1, 1) - flux[c]) for c in range(6)]
        for c in range(6):
            out_ref[c, index] = total[c][:, 0:120]
        return jnp.maximum(fastest, jnp.where(lanes, fastest_signal(total), 0.0))

    fastest = lax.fori_loop(0, 4, final, jnp.zeros((8, 128), jnp.float32))
    signal_ref[...] = jnp.full(signal_ref.shape, jnp.max(fastest))


def hydro_step(column, by_even, own, by_odd, count):
    vmem = pl.BlockSpec(memory_space=pltpu.VMEM)
    blocks = [
        pltpu.with_memory_space_constraint(item, pltpu.VMEM)
        for item in (column, by_even, own, by_odd)
    ]
    return pl.pallas_call(
        kernel,
        in_specs=[vmem] * 4,
        out_specs=[vmem, vmem],
        out_shape=[
            jax.ShapeDtypeStruct((6, 4, 8, 120), jnp.float32),
            jax.ShapeDtypeStruct((count, 1, 1), jnp.float32),
        ],
        scratch_shapes=[
            pltpu.VMEM((6, 12, 16, 128), jnp.float32),
            pltpu.VMEM((3, 6, 6, 16, 128), jnp.float32),
            pltpu.VMEM((3, 6, 6, 16, 128), jnp.float32),
            pltpu.VMEM((3, 6, 6, 16, 128), jnp.float32),
            pltpu.VMEM((6, 5, 8, 128), jnp.float32),
        ],
        name="hydro",
    )(*blocks)


def step(conserved_state):
    tiles = lax.all_to_all(packed(conserved_state), PLANE, 0, 0, tiled=True)
    block, to_column = unpacked(conserved_state, tiles, lax.axis_size(COLUMN))
    column = over_column(to_column, 8)
    block = padded(block, GY, lax.axis_index("x") % 2 == 1, 2, GHOST)
    by_even, by_odd = swapped(block, GX, lax.axis_index("c") == 1, 1, GHOST)
    updated, to_plane = hydro_step(column, by_even, block, by_odd, lax.axis_size(PLANE))
    plane = lax.all_to_all(to_plane, PLANE, 0, 0, tiled=True)
    to_column = spread(plane, lax.axis_size(COLUMN))
    column = lax.all_to_all(to_column, COLUMN, 0, 0, tiled=True)
    return (updated, courant / jnp.max(column))


def solution(mesh):
    finer = Mesh(mesh.devices.reshape(16, 2, 2, 4, 4), ALL)
    spec = P(None, GX, GY, GZ)
    return jax.shard_map(step, mesh=finer, in_specs=(spec,), out_specs=(spec, P()), check_vma=False)
```

```python
import jax
import jax.numpy as jnp
from jax import lax
from jax.experimental import pallas as pl
from jax.experimental.pallas import tpu as pltpu
from jax.sharding import Mesh
from jax.sharding import PartitionSpec as P

GHOST = 4
ALL = ("zl", "c", "zh", "x", "y")
PLANE = ("c", "x", "y")
COLUMN = ("zl", "zh")
GX = ("zl", "c")
GY = ("zh", "x")
GZ = ("y",)

adiabatic = 5.0 / 3.0
courant = 0.3


def over_column(value, first):
    halves, rows = lax.axis_size("zh"), lax.axis_size("zl")
    deep = halves * rows
    order = [(first + step) % deep for step in range(deep)]
    columns, width = lax.axis_size("c"), lax.axis_size(("x", "y"))
    groups = [
        [(((z % rows) * columns + c) * halves + z // rows) * width + place for z in order]
        for c in range(columns)
        for place in range(width)
    ]
    return lax.all_to_all(value, ALL, 0, 0, axis_index_groups=groups, tiled=True)


def swaps(count):
    even = [(i, i ^ 1) for i in range(count)]
    odd = [(i, (i + 1) % count if i % 2 else (i - 1) % count) for i in range(count)]
    return even, odd


def swap(block, axes, odd):
    return lax.ppermute(block, axes, swaps(lax.axis_size(axes))[odd])


def corner_swap():
    sizes = [lax.axis_size(axis) for axis in ALL]
    rows, cores, halves, columns, width = sizes
    _, odd_first = swaps(rows * cores)
    _, odd_second = swaps(halves * columns)
    pairs = []
    for first in range(rows * cores):
        for second in range(halves * columns):
            far_first, far_second = first in (0, rows * cores - 1), second % columns in (0, columns - 1)
            to_first = odd_first[first][1] if far_second else first
            to_second = second if far_second and not far_first else odd_second[second][1]
            if far_first and not far_second:
                to_first = first
            for y in range(width):
                here = (first * halves * columns + second) * width + y
                there = (to_first * halves * columns + to_second) * width + y
                pairs.append((here, there))
    return pairs


def roll(value, shift, axis):
    return pltpu.roll(value, shift % value.shape[axis], axis)


def primitive_of(conserved):
    density, energy = conserved[0], conserved[4]
    inverse = 1.0 / density
    speed = [conserved[component] * inverse for component in (1, 2, 3)]
    kinetic = 0.5 * (conserved[1] * speed[0] + conserved[2] * speed[1] + conserved[3] * speed[2])
    return [density, *speed, (adiabatic - 1.0) * (energy - kinetic), conserved[5] * inverse]


def conserved_of(primitive):
    density = primitive[0]
    momenta = [density * primitive[component] for component in (1, 2, 3)]
    kinetic = 0.5 * (
        momenta[0] * primitive[1] + momenta[1] * primitive[2] + momenta[2] * primitive[3]
    )
    energy = primitive[4] * (1.0 / (adiabatic - 1.0)) + kinetic
    return [density, *momenta, energy, density * primitive[5]]


def fastest_signal(conserved):
    primitive = primitive_of(conserved)
    sound = jnp.sqrt(adiabatic * primitive[4] / primitive[0])
    speeds = jnp.maximum(
        jnp.maximum(jnp.abs(primitive[1]), jnp.abs(primitive[2])), jnp.abs(primitive[3])
    )
    return speeds + sound


def edge_of(q3, q2, q1, q, a1, a2):
    edge = (37.0 / 60.0) * (q1 + q) - (8.0 / 60.0) * (q2 + a1) + (1.0 / 60.0) * (q3 + a2)
    return jnp.clip(edge, jnp.minimum(q1, q), jnp.maximum(q1, q))


def limited(q, lower, upper):
    above, below = upper - q, q - lower
    spread = upper - lower
    skewed = spread * (0.5 * (below - above))
    limit = spread * spread * (1.0 / 6.0)
    flat = above * below <= 0.0
    new_lower = jnp.where(flat, q, jnp.where(skewed > limit, q - 2.0 * above, lower))
    new_upper = jnp.where(flat, q, jnp.where(skewed < -limit, q + 2.0 * below, upper))
    return new_lower, new_upper


def traced(primitive, edges, normal, half_step):
    slopes = [upper - lower for lower, upper in edges]
    density, speed, pressure = primitive[0], primitive[normal], primitive[4]
    rates = [-(speed * slopes[component]) for component in range(6)]
    rates[0] = rates[0] - density * slopes[normal]
    rates[normal] = rates[normal] - slopes[4] / density
    rates[4] = rates[4] - adiabatic * pressure * slopes[normal]
    moves = [half_step * rate for rate in rates]
    lower = [edges[component][0] + moves[component] for component in range(6)]
    upper = [edges[component][1] + moves[component] for component in range(6)]
    return lower, upper


def hllc_flux(left, right, normal):
    ratio_left, ratio_right = left[4] / left[0], right[4] / right[0]
    sound_left, sound_right = jnp.sqrt(adiabatic * ratio_left), jnp.sqrt(adiabatic * ratio_right)
    low = jnp.minimum(left[normal] - sound_left, right[normal] - sound_right)
    high = jnp.maximum(left[normal] + sound_left, right[normal] + sound_right)
    mass_left = left[0] * (low - left[normal])
    mass_right = right[0] * (high - right[normal])
    middle = (right[4] - left[4] + mass_left * left[normal] - mass_right * right[normal]) / (
        mass_left - mass_right
    )
    from_left = middle >= 0.0
    side = [jnp.where(from_left, left[component], right[component]) for component in range(6)]
    ratio = jnp.where(from_left, ratio_left, ratio_right)
    mass = jnp.where(from_left, mass_left, mass_right)
    outer = jnp.where(from_left, low, high)
    weight = jnp.where(from_left, jnp.minimum(low, 0.0), jnp.maximum(high, 0.0))
    speed, pressure = side[normal], side[4]
    state = conserved_of(side)
    flux = [item * speed for item in state]
    flux[normal] = flux[normal] + pressure
    flux[4] = flux[4] + pressure * speed
    factor = mass / (outer - middle)
    star = [factor * item for item in side]
    star[0] = factor
    star[normal] = factor * middle
    half_square = 0.5 * (side[1] * side[1] + side[2] * side[2] + side[3] * side[3])
    specific = ratio * (1.0 / (adiabatic - 1.0)) + half_square
    star[4] = factor * (specific + (middle - speed) * (middle + pressure / mass))
    return [flux[c] + weight * (star[c] - state[c]) for c in range(6)]


def maximum_of(everyone_ref):
    fastest = everyone_ref[0]
    for device in range(1, everyone_ref.shape[0]):
        fastest = jnp.maximum(fastest, everyone_ref[device])
    return fastest


def spread_kernel(everyone_ref, out_ref):
    out_ref[...] = jnp.broadcast_to(maximum_of(everyone_ref)[None], out_ref.shape)


def spread(everyone, count):
    vmem = pl.BlockSpec(memory_space=pltpu.VMEM)
    return pl.pallas_call(
        spread_kernel,
        in_specs=[vmem],
        out_specs=vmem,
        out_shape=jax.ShapeDtypeStruct((count, 1, 1), jnp.float32),
        name="spread",
    )(pltpu.with_memory_space_constraint(everyone, pltpu.VMEM))


def lane_ids():
    return lax.broadcasted_iota(jnp.int32, (8, 128), 1)


def pack_kernel(state_ref, out_ref, wide):
    lanes = lane_ids()
    for c in range(6):
        for layer in range(4):
            wide[c, layer, :, 0:120] = state_ref[c, layer]
    fastest = jnp.zeros((8, 128), jnp.float32)
    for layer in range(4):
        signal = fastest_signal([wide[c, layer] for c in range(6)])
        fastest = jnp.maximum(fastest, jnp.where(lanes < 120, signal, 0.0))
    first = last = jnp.full((8, 128), jnp.max(fastest))
    for c in range(6):
        for layer in range(4):
            spot = 4 * (4 * c + layer)
            here = (lanes >= spot) & (lanes < spot + 4)
            first = jnp.where(here, roll(wide[c, layer], spot, 1), first)
            last = jnp.where(here, roll(wide[c, layer], spot - 116, 1), last)
    above = lax.rem(lax.axis_index("y") + 1, 4)
    for y in range(4):
        tile = jnp.where(above == y, last, first)
        for place in range(y, 32, 4):
            out_ref[place] = tile


def unpack_kernel(state_ref, tiles_ref, block_ref, even_ref, odd_ref, column_ref):
    lanes = lane_ids()
    fastest = tiles_ref[0]
    for place in range(1, 32):
        fastest = jnp.maximum(fastest, tiles_ref[place])
    fastest = jnp.max(jnp.where(lanes >= 96, fastest, 0.0))
    column_ref[...] = jnp.full(column_ref.shape, fastest)
    y = lax.axis_index("y")
    base = 16 * lax.axis_index("c") + 4 * lax.axis_index("x")
    odd = lax.rem(lax.axis_index("x"), 2) == 1
    below = tiles_ref[base + lax.rem(y + 3, 4)]
    above = tiles_ref[base + lax.rem(y + 1, 4)]
    for c in range(6):
        for layer in range(4):
            spot = 4 * (4 * c + layer)
            ghosts = jnp.where(lanes < 124, roll(above, 120 - spot, 1), roll(below, 124 - spot, 1))
            block_ref[c, layer] = ghosts
            block_ref[c, layer, :, 0:120] = state_ref[c, layer]
            whole = block_ref[c, layer]
            first, last = whole[0:4], whole[4:8]
            even_ref[c, layer] = jnp.where(odd, first, last)
            odd_ref[c, layer] = jnp.where(odd, last, first)


def in_vmem(*arrays):
    return [pltpu.with_memory_space_constraint(item, pltpu.VMEM) for item in arrays]


def packed(state):
    vmem = pl.BlockSpec(memory_space=pltpu.VMEM)
    return pl.pallas_call(
        pack_kernel,
        in_specs=[vmem],
        out_specs=vmem,
        out_shape=jax.ShapeDtypeStruct((32, 8, 128), jnp.float32),
        scratch_shapes=[pltpu.VMEM((6, 4, 8, 128), jnp.float32)],
        name="pack",
    )(*in_vmem(state))


def unpacked(state, tiles, count):
    vmem = pl.BlockSpec(memory_space=pltpu.VMEM)
    return pl.pallas_call(
        unpack_kernel,
        in_specs=[vmem] * 2,
        out_specs=[vmem] * 4,
        out_shape=[
            jax.ShapeDtypeStruct((6, 4, 8, 128), jnp.float32),
            jax.ShapeDtypeStruct((6, 4, 4, 128), jnp.float32),
            jax.ShapeDtypeStruct((6, 4, 4, 128), jnp.float32),
            jax.ShapeDtypeStruct((count, 1, 1), jnp.float32),
        ],
        name="unpack",
    )(*in_vmem(state, tiles))


def kernel(column_ref, even_ref, own_ref, odd_ref, out_ref, signal_ref, prim, lower, upper, fluxes, gx):
    step = jnp.max(courant / maximum_of(column_ref))
    half = 0.5 * step
    even_start = 8 - 8 * lax.axis_index("c")
    for source, start in ((even_ref, even_start), (own_ref, 4), (odd_ref, 8 - even_start)):
        for layer in range(4):
            values = primitive_of([source[c, layer] for c in range(6)])
            for c in range(6):
                prim[c, start + layer] = values[c]

    def faces(index, carry):
        own = [prim[c, index + 3] for c in range(6)]
        edges = []
        for c in range(6):
            q = [prim[c, index + k] for k in range(7)]
            edges.append(
                limited(own[c], edge_of(*q[0:6]), edge_of(*q[1:7]))
            )
        for axis in range(3):
            if axis:
                edges = []
                for c in range(6):
                    q = own[c]
                    near = [roll(q, k, axis - 1) for k in (3, 2, 1)]
                    far = [roll(q, -k, axis - 1) for k in (1, 2)]
                    edge = edge_of(*near, q, *far)
                    edges.append(limited(q, edge, roll(edge, -1, axis - 1)))
            low_face, high_face = traced(own, edges, 1 + axis, half)
            for c in range(6):
                lower[axis, c, index] = low_face[c]
                upper[axis, c, index] = high_face[c]
        return carry

    lax.fori_loop(0, 6, faces, 0)

    def predicted(index, carry):
        for axis in (1, 2):
            left = [roll(upper[axis, c, index], 1, axis - 1) for c in range(6)]
            flux = hllc_flux(left, [lower[axis, c, index] for c in range(6)], 1 + axis)
            for c in range(6):
                fluxes[axis, c, index] = half * (roll(flux[c], -1, axis - 1) - flux[c])
        return carry

    lax.fori_loop(0, 6, predicted, 0)

    def predicted_first(index, carry):
        flux = hllc_flux(
            [upper[0, c, index] for c in range(6)], [lower[0, c, index + 1] for c in range(6)], 1
        )
        for c in range(6):
            fluxes[0, c, index] = flux[c]
        return carry

    lax.fori_loop(0, 5, predicted_first, 0)

    def corrected(states, changes):
        state = conserved_of(states)
        return primitive_of([state[c] - changes[c] for c in range(6)])

    def final_first(index, carry):
        change = [fluxes[1, c, index + 1, 0:8] + fluxes[2, c, index + 1, 0:8] for c in range(6)]
        before = [carry[c] for c in range(6)]
        right = corrected([lower[0, c, index + 1, 0:8] for c in range(6)], change)
        flux = hllc_flux(before, right, 1)
        for c in range(6):
            gx[c, index] = flux[c]
        return tuple(corrected([upper[0, c, index + 1, 0:8] for c in range(6)], change))

    change = [fluxes[1, c, 0, 0:8] + fluxes[2, c, 0, 0:8] for c in range(6)]
    first = tuple(corrected([upper[0, c, 0, 0:8] for c in range(6)], change))
    lax.fori_loop(0, 5, final_first, first)

    lanes = lane_ids() < 120

    def final(index, fastest):
        here = index + 1
        total = [own_ref[c, index, 0:8] - step * (gx[c, index + 1] - gx[c, index]) for c in range(6)]
        ahead = [half * (fluxes[0, c, here] - fluxes[0, c, index]) for c in range(6)]
        change = [ahead[c] + fluxes[2, c, here] for c in range(6)]
        left = corrected([upper[1, c, here] for c in range(6)], change)
        right = corrected([lower[1, c, here] for c in range(6)], change)
        flux = hllc_flux([roll(item, 1, 0) for item in left], right, 2)
        total = [total[c] - step * (roll(flux[c], -1, 0)[0:8] - flux[c][0:8]) for c in range(6)]
        change = [ahead[c][0:8] + fluxes[1, c, here, 0:8] for c in range(6)]
        left = corrected([upper[2, c, here, 0:8] for c in range(6)], change)
        right = corrected([lower[2, c, here, 0:8] for c in range(6)], change)
        flux = hllc_flux([roll(item, 1, 1) for item in left], right, 3)
        total = [total[c] - step * (roll(flux[c], -1, 1) - flux[c]) for c in range(6)]
        for c in range(6):
            out_ref[c, index] = total[c][:, 0:120]
        return jnp.maximum(fastest, jnp.where(lanes, fastest_signal(total), 0.0))

    fastest = lax.fori_loop(0, 4, final, jnp.zeros((8, 128), jnp.float32))
    signal_ref[...] = jnp.full(signal_ref.shape, jnp.max(fastest))


def hydro_step(column, by_even, own, by_odd, count):
    vmem = pl.BlockSpec(memory_space=pltpu.VMEM)
    blocks = [
        pltpu.with_memory_space_constraint(item, pltpu.VMEM)
        for item in (column, by_even, own, by_odd)
    ]
    return pl.pallas_call(
        kernel,
        in_specs=[vmem] * 4,
        out_specs=[vmem, vmem],
        out_shape=[
            jax.ShapeDtypeStruct((6, 4, 8, 120), jnp.float32),
            jax.ShapeDtypeStruct((count, 1, 1), jnp.float32),
        ],
        scratch_shapes=[
            pltpu.VMEM((6, 12, 16, 128), jnp.float32),
            pltpu.VMEM((3, 6, 6, 16, 128), jnp.float32),
            pltpu.VMEM((3, 6, 6, 16, 128), jnp.float32),
            pltpu.VMEM((3, 6, 6, 16, 128), jnp.float32),
            pltpu.VMEM((6, 5, 8, 128), jnp.float32),
        ],
        name="hydro",
    )(*blocks)


def cyclic(block, by_even, by_odd, odd):
    above, below = jnp.where(odd, by_odd, by_even), jnp.where(odd, by_even, by_odd)
    return jnp.concatenate([block, above, below], axis=2)


def step(conserved_state):
    tiles = lax.all_to_all(packed(conserved_state), PLANE, 0, 0, tiled=True)
    block, to_even, to_odd, to_column = unpacked(
        conserved_state, tiles, lax.axis_size(COLUMN)
    )
    x, chip_row, core = (lax.axis_index(axis) for axis in ("x", "zl", "c"))
    odd = x % 2 == 1
    far_second = (x == 0) | (x == lax.axis_size("x") - 1)
    far_first = ((core == 0) & (chip_row == 0)) | ((core == 1) & (chip_row == lax.axis_size("zl") - 1))
    beside_odd = swap(to_odd, GY, 1)
    ahead_odd = swap(block, GX, 1)
    beside_even = swap(to_even, GY, 0)
    column = over_column(to_column, 8)
    own = cyclic(block, beside_even, beside_odd, odd)
    by_even = swap(own, GX, 0)
    low, high = ahead_odd[:, :, :GHOST], ahead_odd[:, :, GHOST:]
    corner_even = swap(jnp.where(odd, low, high), GY, 0)
    kept = jnp.where(far_first, to_odd, beside_odd)
    corner_odd = lax.ppermute(
        jnp.where(far_second, kept, jnp.where(odd, high, low)), ALL, corner_swap()
    )
    by_odd = cyclic(ahead_odd, corner_even, corner_odd, odd)
    updated, to_plane = hydro_step(column, by_even, own, by_odd, lax.axis_size(PLANE))
    plane = lax.all_to_all(to_plane, PLANE, 0, 0, tiled=True)
    to_column = spread(plane, lax.axis_size(COLUMN))
    column = lax.all_to_all(to_column, COLUMN, 0, 0, tiled=True)
    return (updated, courant / jnp.max(column))


def solution(mesh):
    finer = Mesh(mesh.devices.reshape(16, 2, 2, 4, 4), ALL)
    spec = P(None, GX, GY, GZ)
    return jax.shard_map(step, mesh=finer, in_specs=(spec,), out_specs=(spec, P()), check_vma=False)
```

```python
import jax
import jax.numpy as jnp
from jax import lax
from jax.experimental import pallas as pl
from jax.experimental.pallas import tpu as pltpu
from jax.sharding import Mesh
from jax.sharding import PartitionSpec as P

GHOST = 4
ALL = ("zl", "c", "zh", "x", "y")
PLANE = ("c", "x", "y")
COLUMN = ("zl", "zh")
GX = ("zl", "c")
GY = ("zh", "x")
GZ = ("y",)

adiabatic = 5.0 / 3.0
courant = 0.3


def over_column(value, first):
    halves, rows = lax.axis_size("zh"), lax.axis_size("zl")
    deep = halves * rows
    order = [(first + step) % deep for step in range(deep)]
    columns, width = lax.axis_size("c"), lax.axis_size(("x", "y"))
    groups = [
        [(((z % rows) * columns + c) * halves + z // rows) * width + place for z in order]
        for c in range(columns)
        for place in range(width)
    ]
    return lax.all_to_all(value, ALL, 0, 0, axis_index_groups=groups, tiled=True)


def swaps(count):
    even = [(i, i ^ 1) for i in range(count)]
    odd = [(i, (i + 1) % count if i % 2 else (i - 1) % count) for i in range(count)]
    return even, odd


def swap(block, axes, odd):
    return lax.ppermute(block, axes, swaps(lax.axis_size(axes))[odd])


def corner_swap():
    sizes = [lax.axis_size(axis) for axis in ALL]
    rows, cores, halves, columns, width = sizes
    _, odd_first = swaps(rows * cores)
    _, odd_second = swaps(halves * columns)
    pairs = []
    for first in range(rows * cores):
        for second in range(halves * columns):
            far_first, far_second = first in (0, rows * cores - 1), second % columns in (0, columns - 1)
            to_first = odd_first[first][1] if far_second else first
            to_second = second if far_second and not far_first else odd_second[second][1]
            if far_first and not far_second:
                to_first = first
            for y in range(width):
                here = (first * halves * columns + second) * width + y
                there = (to_first * halves * columns + to_second) * width + y
                pairs.append((here, there))
    return pairs


def roll(value, shift, axis):
    return pltpu.roll(value, shift % value.shape[axis], axis)


def primitive_of(conserved):
    density, energy = conserved[0], conserved[4]
    inverse = 1.0 / density
    speed = [conserved[component] * inverse for component in (1, 2, 3)]
    kinetic = 0.5 * (conserved[1] * speed[0] + conserved[2] * speed[1] + conserved[3] * speed[2])
    return [density, *speed, (adiabatic - 1.0) * (energy - kinetic), conserved[5] * inverse]


def conserved_of(primitive):
    density = primitive[0]
    momenta = [density * primitive[component] for component in (1, 2, 3)]
    kinetic = 0.5 * (
        momenta[0] * primitive[1] + momenta[1] * primitive[2] + momenta[2] * primitive[3]
    )
    energy = primitive[4] * (1.0 / (adiabatic - 1.0)) + kinetic
    return [density, *momenta, energy, density * primitive[5]]


def fastest_signal(conserved):
    primitive = primitive_of(conserved)
    sound = jnp.sqrt(adiabatic * primitive[4] / primitive[0])
    speeds = jnp.maximum(
        jnp.maximum(jnp.abs(primitive[1]), jnp.abs(primitive[2])), jnp.abs(primitive[3])
    )
    return speeds + sound


def edge_of(q3, q2, q1, q, a1, a2):
    edge = (37.0 / 60.0) * (q1 + q) - (8.0 / 60.0) * (q2 + a1) + (1.0 / 60.0) * (q3 + a2)
    return jnp.clip(edge, jnp.minimum(q1, q), jnp.maximum(q1, q))


def limited(q, lower, upper):
    above, below = upper - q, q - lower
    spread = upper - lower
    skewed = spread * (0.5 * (below - above))
    limit = spread * spread * (1.0 / 6.0)
    flat = above * below <= 0.0
    new_lower = jnp.where(flat, q, jnp.where(skewed > limit, q - 2.0 * above, lower))
    new_upper = jnp.where(flat, q, jnp.where(skewed < -limit, q + 2.0 * below, upper))
    return new_lower, new_upper


def traced(primitive, edges, normal, half_step):
    slopes = [upper - lower for lower, upper in edges]
    density, speed, pressure = primitive[0], primitive[normal], primitive[4]
    rates = [-(speed * slopes[component]) for component in range(6)]
    rates[0] = rates[0] - density * slopes[normal]
    rates[normal] = rates[normal] - slopes[4] / density
    rates[4] = rates[4] - adiabatic * pressure * slopes[normal]
    moves = [half_step * rate for rate in rates]
    lower = [edges[component][0] + moves[component] for component in range(6)]
    upper = [edges[component][1] + moves[component] for component in range(6)]
    return lower, upper


def hllc_flux(left, right, normal):
    ratio_left, ratio_right = left[4] / left[0], right[4] / right[0]
    sound_left, sound_right = jnp.sqrt(adiabatic * ratio_left), jnp.sqrt(adiabatic * ratio_right)
    low = jnp.minimum(left[normal] - sound_left, right[normal] - sound_right)
    high = jnp.maximum(left[normal] + sound_left, right[normal] + sound_right)
    mass_left = left[0] * (low - left[normal])
    mass_right = right[0] * (high - right[normal])
    middle = (right[4] - left[4] + mass_left * left[normal] - mass_right * right[normal]) / (
        mass_left - mass_right
    )
    from_left = middle >= 0.0
    side = [jnp.where(from_left, left[component], right[component]) for component in range(6)]
    ratio = jnp.where(from_left, ratio_left, ratio_right)
    mass = jnp.where(from_left, mass_left, mass_right)
    outer = jnp.where(from_left, low, high)
    weight = jnp.where(from_left, jnp.minimum(low, 0.0), jnp.maximum(high, 0.0))
    speed, pressure = side[normal], side[4]
    state = conserved_of(side)
    flux = [item * speed for item in state]
    flux[normal] = flux[normal] + pressure
    flux[4] = flux[4] + pressure * speed
    factor = mass / (outer - middle)
    star = [factor * item for item in side]
    star[0] = factor
    star[normal] = factor * middle
    half_square = 0.5 * (side[1] * side[1] + side[2] * side[2] + side[3] * side[3])
    specific = ratio * (1.0 / (adiabatic - 1.0)) + half_square
    star[4] = factor * (specific + (middle - speed) * (middle + pressure / mass))
    return [flux[c] + weight * (star[c] - state[c]) for c in range(6)]


def maximum_of(everyone_ref):
    fastest = everyone_ref[0]
    for device in range(1, everyone_ref.shape[0]):
        fastest = jnp.maximum(fastest, everyone_ref[device])
    return fastest


def spread_kernel(everyone_ref, out_ref):
    out_ref[...] = jnp.broadcast_to(maximum_of(everyone_ref)[None], out_ref.shape)


def spread(everyone, count):
    vmem = pl.BlockSpec(memory_space=pltpu.VMEM)
    return pl.pallas_call(
        spread_kernel,
        in_specs=[vmem],
        out_specs=vmem,
        out_shape=pltpu.VMEM((count, 1, 1), jnp.float32),
        name="spread",
    )(pltpu.with_memory_space_constraint(everyone, pltpu.VMEM))


def lane_ids():
    return lax.broadcasted_iota(jnp.int32, (8, 128), 1)


def pack_kernel(state_ref, out_ref, wide):
    lanes = lane_ids()
    for c in range(6):
        for layer in range(4):
            wide[c, layer, :, 0:120] = state_ref[c, layer]
    fastest = jnp.zeros((8, 128), jnp.float32)
    for layer in range(4):
        signal = fastest_signal([wide[c, layer] for c in range(6)])
        fastest = jnp.maximum(fastest, jnp.where(lanes < 120, signal, 0.0))
    first = last = jnp.full((8, 128), jnp.max(fastest))
    for c in range(6):
        for layer in range(4):
            spot = 4 * (4 * c + layer)
            here = (lanes >= spot) & (lanes < spot + 4)
            first = jnp.where(here, roll(wide[c, layer], spot, 1), first)
            last = jnp.where(here, roll(wide[c, layer], spot - 116, 1), last)
    above = lax.rem(lax.axis_index("y") + 1, 4)
    for y in range(4):
        tile = jnp.where(above == y, last, first)
        for place in range(y, 32, 4):
            out_ref[place] = tile


def unpack_kernel(state_ref, tiles_ref, block_ref, even_ref, odd_ref, column_ref):
    lanes = lane_ids()
    fastest = tiles_ref[0]
    for place in range(1, 32):
        fastest = jnp.maximum(fastest, tiles_ref[place])
    fastest = jnp.max(jnp.where(lanes >= 96, fastest, 0.0))
    column_ref[...] = jnp.full(column_ref.shape, fastest)
    y = lax.axis_index("y")
    base = 16 * lax.axis_index("c") + 4 * lax.axis_index("x")
    odd = lax.rem(lax.axis_index("x"), 2) == 1
    below = tiles_ref[base + lax.rem(y + 3, 4)]
    above = tiles_ref[base + lax.rem(y + 1, 4)]
    for c in range(6):
        for layer in range(4):
            spot = 4 * (4 * c + layer)
            ghosts = jnp.where(lanes < 124, roll(above, 120 - spot, 1), roll(below, 124 - spot, 1))
            block_ref[c, layer] = ghosts
            block_ref[c, layer, :, 0:120] = state_ref[c, layer]
            whole = block_ref[c, layer]
            first, last = whole[0:4], whole[4:8]
            even_ref[c, layer] = jnp.where(odd, first, last)
            odd_ref[c, layer] = jnp.where(odd, last, first)


def in_vmem(*arrays):
    return [pltpu.with_memory_space_constraint(item, pltpu.VMEM) for item in arrays]


def packed(state):
    vmem = pl.BlockSpec(memory_space=pltpu.VMEM)
    return pl.pallas_call(
        pack_kernel,
        in_specs=[vmem],
        out_specs=vmem,
        out_shape=jax.ShapeDtypeStruct((32, 8, 128), jnp.float32),
        scratch_shapes=[pltpu.VMEM((6, 4, 8, 128), jnp.float32)],
        name="pack",
    )(*in_vmem(state))


def unpacked(state, tiles, count):
    vmem = pl.BlockSpec(memory_space=pltpu.VMEM)
    return pl.pallas_call(
        unpack_kernel,
        in_specs=[vmem] * 2,
        out_specs=[vmem] * 4,
        out_shape=[
            pltpu.VMEM((6, 4, 8, 128), jnp.float32),
            pltpu.VMEM((6, 4, 4, 128), jnp.float32),
            pltpu.VMEM((6, 4, 4, 128), jnp.float32),
            jax.ShapeDtypeStruct((count, 1, 1), jnp.float32),
        ],
        name="unpack",
    )(*in_vmem(state, tiles))


def kernel(column_ref, even_ref, own_ref, odd_ref, out_ref, signal_ref, prim, lower, upper, fluxes, gx):
    step = jnp.max(courant / maximum_of(column_ref))
    half = 0.5 * step
    even_start = 8 - 8 * lax.axis_index("c")
    for source, start in ((even_ref, even_start), (own_ref, 4), (odd_ref, 8 - even_start)):
        for layer in range(4):
            values = primitive_of([source[c, layer] for c in range(6)])
            for c in range(6):
                prim[c, start + layer] = values[c]

    def faces(index, carry):
        own = [prim[c, index + 3] for c in range(6)]
        edges = []
        for c in range(6):
            q = [prim[c, index + k] for k in range(7)]
            edges.append(
                limited(own[c], edge_of(*q[0:6]), edge_of(*q[1:7]))
            )
        for axis in range(3):
            if axis:
                edges = []
                for c in range(6):
                    q = own[c]
                    near = [roll(q, k, axis - 1) for k in (3, 2, 1)]
                    far = [roll(q, -k, axis - 1) for k in (1, 2)]
                    edge = edge_of(*near, q, *far)
                    edges.append(limited(q, edge, roll(edge, -1, axis - 1)))
            low_face, high_face = traced(own, edges, 1 + axis, half)
            for c in range(6):
                lower[axis, c, index] = low_face[c]
                upper[axis, c, index] = high_face[c]
        return carry

    lax.fori_loop(0, 6, faces, 0)

    def predicted(index, carry):
        for axis in (1, 2):
            left = [roll(upper[axis, c, index], 1, axis - 1) for c in range(6)]
            flux = hllc_flux(left, [lower[axis, c, index] for c in range(6)], 1 + axis)
            for c in range(6):
                fluxes[axis, c, index] = half * (roll(flux[c], -1, axis - 1) - flux[c])
        return carry

    lax.fori_loop(0, 6, predicted, 0)

    def predicted_first(index, carry):
        flux = hllc_flux(
            [upper[0, c, index] for c in range(6)], [lower[0, c, index + 1] for c in range(6)], 1
        )
        for c in range(6):
            fluxes[0, c, index] = flux[c]
        return carry

    lax.fori_loop(0, 5, predicted_first, 0)

    def corrected(states, changes):
        state = conserved_of(states)
        return primitive_of([state[c] - changes[c] for c in range(6)])

    def final_first(index, carry):
        change = [fluxes[1, c, index + 1, 0:8] + fluxes[2, c, index + 1, 0:8] for c in range(6)]
        before = [carry[c] for c in range(6)]
        right = corrected([lower[0, c, index + 1, 0:8] for c in range(6)], change)
        flux = hllc_flux(before, right, 1)
        for c in range(6):
            gx[c, index] = flux[c]
        return tuple(corrected([upper[0, c, index + 1, 0:8] for c in range(6)], change))

    change = [fluxes[1, c, 0, 0:8] + fluxes[2, c, 0, 0:8] for c in range(6)]
    first = tuple(corrected([upper[0, c, 0, 0:8] for c in range(6)], change))
    lax.fori_loop(0, 5, final_first, first)

    lanes = lane_ids() < 120

    def final(index, fastest):
        here = index + 1
        total = [own_ref[c, index, 0:8] - step * (gx[c, index + 1] - gx[c, index]) for c in range(6)]
        ahead = [half * (fluxes[0, c, here] - fluxes[0, c, index]) for c in range(6)]
        change = [ahead[c] + fluxes[2, c, here] for c in range(6)]
        left = corrected([upper[1, c, here] for c in range(6)], change)
        right = corrected([lower[1, c, here] for c in range(6)], change)
        flux = hllc_flux([roll(item, 1, 0) for item in left], right, 2)
        total = [total[c] - step * (roll(flux[c], -1, 0)[0:8] - flux[c][0:8]) for c in range(6)]
        change = [ahead[c][0:8] + fluxes[1, c, here, 0:8] for c in range(6)]
        left = corrected([upper[2, c, here, 0:8] for c in range(6)], change)
        right = corrected([lower[2, c, here, 0:8] for c in range(6)], change)
        flux = hllc_flux([roll(item, 1, 1) for item in left], right, 3)
        total = [total[c] - step * (roll(flux[c], -1, 1) - flux[c]) for c in range(6)]
        for c in range(6):
            out_ref[c, index] = total[c][:, 0:120]
        return jnp.maximum(fastest, jnp.where(lanes, fastest_signal(total), 0.0))

    fastest = lax.fori_loop(0, 4, final, jnp.zeros((8, 128), jnp.float32))
    signal_ref[...] = jnp.full(signal_ref.shape, jnp.max(fastest))


def hydro_step(column, by_even, own, by_odd, count):
    vmem = pl.BlockSpec(memory_space=pltpu.VMEM)
    blocks = [
        pltpu.with_memory_space_constraint(item, pltpu.VMEM)
        for item in (column, by_even, own, by_odd)
    ]
    return pl.pallas_call(
        kernel,
        in_specs=[vmem] * 4,
        out_specs=[vmem, vmem],
        out_shape=[
            pltpu.VMEM((6, 4, 8, 120), jnp.float32),
            pltpu.VMEM((count, 1, 1), jnp.float32),
        ],
        scratch_shapes=[
            pltpu.VMEM((6, 12, 16, 128), jnp.float32),
            pltpu.VMEM((3, 6, 6, 16, 128), jnp.float32),
            pltpu.VMEM((3, 6, 6, 16, 128), jnp.float32),
            pltpu.VMEM((3, 6, 6, 16, 128), jnp.float32),
            pltpu.VMEM((6, 5, 8, 128), jnp.float32),
        ],
        name="hydro",
    )(*blocks)


def cyclic(block, by_even, by_odd, odd):
    above, below = jnp.where(odd, by_odd, by_even), jnp.where(odd, by_even, by_odd)
    return jnp.concatenate([block, above, below], axis=2)


def step(conserved_state):
    tiles = lax.all_to_all(packed(conserved_state), PLANE, 0, 0, tiled=True)
    block, to_even, to_odd, to_column = unpacked(
        conserved_state, tiles, lax.axis_size(COLUMN)
    )
    x, chip_row, core = (lax.axis_index(axis) for axis in ("x", "zl", "c"))
    odd = x % 2 == 1
    far_second = (x == 0) | (x == lax.axis_size("x") - 1)
    far_first = ((core == 0) & (chip_row == 0)) | ((core == 1) & (chip_row == lax.axis_size("zl") - 1))
    beside_odd = swap(to_odd, GY, 1)
    ahead_odd = swap(block, GX, 1)
    beside_even = swap(to_even, GY, 0)
    column = over_column(to_column, 8)
    own = cyclic(block, beside_even, beside_odd, odd)
    by_even = swap(own, GX, 0)
    low, high = ahead_odd[:, :, :GHOST], ahead_odd[:, :, GHOST:]
    corner_even = swap(jnp.where(odd, low, high), GY, 0)
    kept = jnp.where(far_first, to_odd, beside_odd)
    corner_odd = lax.ppermute(
        jnp.where(far_second, kept, jnp.where(odd, high, low)), ALL, corner_swap()
    )
    by_odd = cyclic(ahead_odd, corner_even, corner_odd, odd)
    updated, to_plane = hydro_step(column, by_even, own, by_odd, lax.axis_size(PLANE))
    plane = lax.all_to_all(to_plane, PLANE, 0, 0, tiled=True)
    to_column = spread(plane, lax.axis_size(COLUMN))
    column = lax.all_to_all(to_column, COLUMN, 0, 0, tiled=True)
    return (updated, courant / jnp.max(column))


def solution(mesh):
    finer = Mesh(mesh.devices.reshape(16, 2, 2, 4, 4), ALL)
    spec = P(None, GX, GY, GZ)
    return jax.shard_map(step, mesh=finer, in_specs=(spec,), out_specs=(spec, P()), check_vma=False)
```

```python
import jax
import jax.numpy as jnp
from jax import lax
from jax.experimental import pallas as pl
from jax.experimental.pallas import tpu as pltpu
from jax.sharding import Mesh
from jax.sharding import PartitionSpec as P

GHOST = 4
ALL = ("zl", "c", "zh", "x", "y")
PLANE = ("c", "x", "y")
COLUMN = ("zl", "zh")
GX = ("zl", "c")
GY = ("zh", "x")
GZ = ("y",)

adiabatic = 5.0 / 3.0
courant = 0.3


def over_column(value, first):
    halves, rows = lax.axis_size("zh"), lax.axis_size("zl")
    deep = halves * rows
    order = [(first + step) % deep for step in range(deep)]
    columns, width = lax.axis_size("c"), lax.axis_size(("x", "y"))
    groups = [
        [(((z % rows) * columns + c) * halves + z // rows) * width + place for z in order]
        for c in range(columns)
        for place in range(width)
    ]
    return lax.all_to_all(value, ALL, 0, 0, axis_index_groups=groups, tiled=True)


def swaps(count):
    even = [(i, i ^ 1) for i in range(count)]
    odd = [(i, (i + 1) % count if i % 2 else (i - 1) % count) for i in range(count)]
    return even, odd


def swap(block, axes, odd):
    return lax.ppermute(block, axes, swaps(lax.axis_size(axes))[odd])


def corner_swap():
    sizes = [lax.axis_size(axis) for axis in ALL]
    rows, cores, halves, columns, width = sizes
    _, odd_first = swaps(rows * cores)
    _, odd_second = swaps(halves * columns)
    pairs = []
    for first in range(rows * cores):
        for second in range(halves * columns):
            far_first, far_second = first in (0, rows * cores - 1), second % columns in (0, columns - 1)
            to_first = odd_first[first][1] if far_second else first
            to_second = second if far_second and not far_first else odd_second[second][1]
            if far_first and not far_second:
                to_first = first
            for y in range(width):
                here = (first * halves * columns + second) * width + y
                there = (to_first * halves * columns + to_second) * width + y
                pairs.append((here, there))
    return pairs


def roll(value, shift, axis):
    return pltpu.roll(value, shift % value.shape[axis], axis)


def primitive_of(conserved):
    density, energy = conserved[0], conserved[4]
    inverse = 1.0 / density
    speed = [conserved[component] * inverse for component in (1, 2, 3)]
    kinetic = 0.5 * (conserved[1] * speed[0] + conserved[2] * speed[1] + conserved[3] * speed[2])
    return [density, *speed, (adiabatic - 1.0) * (energy - kinetic), conserved[5] * inverse]


def conserved_of(primitive):
    density = primitive[0]
    momenta = [density * primitive[component] for component in (1, 2, 3)]
    kinetic = 0.5 * (
        momenta[0] * primitive[1] + momenta[1] * primitive[2] + momenta[2] * primitive[3]
    )
    energy = primitive[4] * (1.0 / (adiabatic - 1.0)) + kinetic
    return [density, *momenta, energy, density * primitive[5]]


def fastest_signal(conserved):
    primitive = primitive_of(conserved)
    sound = jnp.sqrt(adiabatic * primitive[4] / primitive[0])
    speeds = jnp.maximum(
        jnp.maximum(jnp.abs(primitive[1]), jnp.abs(primitive[2])), jnp.abs(primitive[3])
    )
    return speeds + sound


def edge_of(q3, q2, q1, q, a1, a2):
    edge = (37.0 / 60.0) * (q1 + q) - (8.0 / 60.0) * (q2 + a1) + (1.0 / 60.0) * (q3 + a2)
    return jnp.clip(edge, jnp.minimum(q1, q), jnp.maximum(q1, q))


def limited(q, lower, upper):
    above, below = upper - q, q - lower
    spread = upper - lower
    skewed = spread * (0.5 * (below - above))
    limit = spread * spread * (1.0 / 6.0)
    flat = above * below <= 0.0
    new_lower = jnp.where(flat, q, jnp.where(skewed > limit, q - 2.0 * above, lower))
    new_upper = jnp.where(flat, q, jnp.where(skewed < -limit, q + 2.0 * below, upper))
    return new_lower, new_upper


def traced(primitive, edges, normal, half_step):
    slopes = [upper - lower for lower, upper in edges]
    density, speed, pressure = primitive[0], primitive[normal], primitive[4]
    rates = [-(speed * slopes[component]) for component in range(6)]
    rates[0] = rates[0] - density * slopes[normal]
    rates[normal] = rates[normal] - slopes[4] / density
    rates[4] = rates[4] - adiabatic * pressure * slopes[normal]
    moves = [half_step * rate for rate in rates]
    lower = [edges[component][0] + moves[component] for component in range(6)]
    upper = [edges[component][1] + moves[component] for component in range(6)]
    return lower, upper


def hllc_flux(left, right, normal):
    ratio_left, ratio_right = left[4] / left[0], right[4] / right[0]
    sound_left, sound_right = jnp.sqrt(adiabatic * ratio_left), jnp.sqrt(adiabatic * ratio_right)
    low = jnp.minimum(left[normal] - sound_left, right[normal] - sound_right)
    high = jnp.maximum(left[normal] + sound_left, right[normal] + sound_right)
    mass_left = left[0] * (low - left[normal])
    mass_right = right[0] * (high - right[normal])
    middle = (right[4] - left[4] + mass_left * left[normal] - mass_right * right[normal]) / (
        mass_left - mass_right
    )
    from_left = middle >= 0.0
    side = [jnp.where(from_left, left[component], right[component]) for component in range(6)]
    ratio = jnp.where(from_left, ratio_left, ratio_right)
    mass = jnp.where(from_left, mass_left, mass_right)
    outer = jnp.where(from_left, low, high)
    weight = jnp.where(from_left, jnp.minimum(low, 0.0), jnp.maximum(high, 0.0))
    speed, pressure = side[normal], side[4]
    state = conserved_of(side)
    flux = [item * speed for item in state]
    flux[normal] = flux[normal] + pressure
    flux[4] = flux[4] + pressure * speed
    factor = mass / (outer - middle)
    star = [factor * item for item in side]
    star[0] = factor
    star[normal] = factor * middle
    half_square = 0.5 * (side[1] * side[1] + side[2] * side[2] + side[3] * side[3])
    specific = ratio * (1.0 / (adiabatic - 1.0)) + half_square
    star[4] = factor * (specific + (middle - speed) * (middle + pressure / mass))
    return [flux[c] + weight * (star[c] - state[c]) for c in range(6)]


def maximum_of(everyone_ref):
    fastest = everyone_ref[0]
    for device in range(1, everyone_ref.shape[0]):
        fastest = jnp.maximum(fastest, everyone_ref[device])
    return fastest


def spread_kernel(everyone_ref, out_ref):
    out_ref[...] = jnp.broadcast_to(maximum_of(everyone_ref)[None], out_ref.shape)


def spread(everyone, count):
    vmem = pl.BlockSpec(memory_space=pltpu.VMEM)
    return pl.pallas_call(
        spread_kernel,
        in_specs=[vmem],
        out_specs=vmem,
        out_shape=pltpu.VMEM((count, 1, 1), jnp.float32),
        name="spread",
    )(pltpu.with_memory_space_constraint(everyone, pltpu.VMEM))


def lane_ids():
    return lax.broadcasted_iota(jnp.int32, (8, 128), 1)


def pack_kernel(state_ref, out_ref, wide):
    lanes = lane_ids()
    for c in range(6):
        for layer in range(4):
            wide[c, layer, :, 0:120] = state_ref[c, layer]
    fastest = jnp.zeros((8, 128), jnp.float32)
    for layer in range(4):
        signal = fastest_signal([wide[c, layer] for c in range(6)])
        fastest = jnp.maximum(fastest, jnp.where(lanes < 120, signal, 0.0))
    first = last = jnp.full((8, 128), jnp.max(fastest))
    for c in range(6):
        for layer in range(4):
            spot = 4 * (4 * c + layer)
            here = (lanes >= spot) & (lanes < spot + 4)
            first = jnp.where(here, roll(wide[c, layer], spot, 1), first)
            last = jnp.where(here, roll(wide[c, layer], spot - 116, 1), last)
    above = lax.rem(lax.axis_index("y") + 1, 4)
    for y in range(4):
        tile = jnp.where(above == y, last, first)
        for place in range(y, 32, 4):
            out_ref[place] = tile


def unpack_kernel(state_ref, tiles_ref, block_ref, even_ref, odd_ref, column_ref):
    lanes = lane_ids()
    fastest = tiles_ref[0]
    for place in range(1, 32):
        fastest = jnp.maximum(fastest, tiles_ref[place])
    fastest = jnp.max(jnp.where(lanes >= 96, fastest, 0.0))
    column_ref[...] = jnp.full(column_ref.shape, fastest)
    y = lax.axis_index("y")
    base = 16 * lax.axis_index("c") + 4 * lax.axis_index("x")
    odd = lax.rem(lax.axis_index("x"), 2) == 1
    below = tiles_ref[base + lax.rem(y + 3, 4)]
    above = tiles_ref[base + lax.rem(y + 1, 4)]
    for c in range(6):
        for layer in range(4):
            spot = 4 * (4 * c + layer)
            ghosts = jnp.where(lanes < 124, roll(above, 120 - spot, 1), roll(below, 124 - spot, 1))
            block_ref[c, layer] = ghosts
            block_ref[c, layer, :, 0:120] = state_ref[c, layer]
            whole = block_ref[c, layer]
            first, last = whole[0:4], whole[4:8]
            even_ref[c, layer] = jnp.where(odd, first, last)
            odd_ref[c, layer] = jnp.where(odd, last, first)


def in_vmem(*arrays):
    return [pltpu.with_memory_space_constraint(item, pltpu.VMEM) for item in arrays]


def packed(state):
    vmem = pl.BlockSpec(memory_space=pltpu.VMEM)
    return pl.pallas_call(
        pack_kernel,
        in_specs=[vmem],
        out_specs=vmem,
        out_shape=jax.ShapeDtypeStruct((32, 8, 128), jnp.float32),
        scratch_shapes=[pltpu.VMEM((6, 4, 8, 128), jnp.float32)],
        name="pack",
    )(*in_vmem(state))


def unpacked(state, tiles, count):
    vmem = pl.BlockSpec(memory_space=pltpu.VMEM)
    return pl.pallas_call(
        unpack_kernel,
        in_specs=[vmem] * 2,
        out_specs=[vmem] * 4,
        out_shape=[
            pltpu.VMEM((6, 4, 8, 128), jnp.float32),
            pltpu.VMEM((6, 4, 4, 128), jnp.float32),
            pltpu.VMEM((6, 4, 4, 128), jnp.float32),
            jax.ShapeDtypeStruct((count, 1, 1), jnp.float32),
        ],
        name="unpack",
    )(*in_vmem(state, tiles))


def kernel(column_ref, even_ref, own_ref, odd_ref, out_ref, signal_ref, prim, lower, upper, fluxes, gx):
    step = jnp.max(courant / maximum_of(column_ref))
    half = 0.5 * step
    even_start = 8 - 8 * lax.axis_index("c")
    for source, start in ((even_ref, even_start), (own_ref, 4), (odd_ref, 8 - even_start)):
        for layer in range(4):
            values = primitive_of([source[c, layer] for c in range(6)])
            for c in range(6):
                prim[c, start + layer] = values[c]

    def faces(index, carry):
        own = [prim[c, index + 3] for c in range(6)]
        edges = []
        for c in range(6):
            q = [prim[c, index + k] for k in range(7)]
            edges.append(
                limited(own[c], edge_of(*q[0:6]), edge_of(*q[1:7]))
            )
        for axis in range(3):
            if axis:
                edges = []
                for c in range(6):
                    q = own[c]
                    near = [roll(q, k, axis - 1) for k in (3, 2, 1)]
                    far = [roll(q, -k, axis - 1) for k in (1, 2)]
                    edge = edge_of(*near, q, *far)
                    edges.append(limited(q, edge, roll(edge, -1, axis - 1)))
            low_face, high_face = traced(own, edges, 1 + axis, half)
            for c in range(6):
                lower[axis, c, index] = low_face[c]
                upper[axis, c, index] = high_face[c]
        return carry

    lax.fori_loop(0, 6, faces, 0)

    def predicted(index, carry):
        for axis in (1, 2):
            left = [roll(upper[axis, c, index], 1, axis - 1) for c in range(6)]
            flux = hllc_flux(left, [lower[axis, c, index] for c in range(6)], 1 + axis)
            for c in range(6):
                fluxes[axis, c, index] = half * (roll(flux[c], -1, axis - 1) - flux[c])
        return carry

    lax.fori_loop(0, 6, predicted, 0)

    def predicted_first(index, carry):
        flux = hllc_flux(
            [upper[0, c, index] for c in range(6)], [lower[0, c, index + 1] for c in range(6)], 1
        )
        for c in range(6):
            fluxes[0, c, index] = flux[c]
        return carry

    lax.fori_loop(0, 5, predicted_first, 0)

    def corrected(states, changes):
        state = conserved_of(states)
        return primitive_of([state[c] - changes[c] for c in range(6)])

    def final_first(index, carry):
        change = [fluxes[1, c, index + 1, 0:8] + fluxes[2, c, index + 1, 0:8] for c in range(6)]
        before = [carry[c] for c in range(6)]
        right = corrected([lower[0, c, index + 1, 0:8] for c in range(6)], change)
        flux = hllc_flux(before, right, 1)
        for c in range(6):
            gx[c, index] = flux[c]
        return tuple(corrected([upper[0, c, index + 1, 0:8] for c in range(6)], change))

    change = [fluxes[1, c, 0, 0:8] + fluxes[2, c, 0, 0:8] for c in range(6)]
    first = tuple(corrected([upper[0, c, 0, 0:8] for c in range(6)], change))
    lax.fori_loop(0, 5, final_first, first)

    lanes = lane_ids() < 120

    def final(index, fastest):
        here = index + 1
        total = [own_ref[c, index, 0:8] - step * (gx[c, index + 1] - gx[c, index]) for c in range(6)]
        ahead = [half * (fluxes[0, c, here] - fluxes[0, c, index]) for c in range(6)]
        change = [ahead[c] + fluxes[2, c, here] for c in range(6)]
        left = corrected([upper[1, c, here] for c in range(6)], change)
        right = corrected([lower[1, c, here] for c in range(6)], change)
        flux = hllc_flux([roll(item, 1, 0) for item in left], right, 2)
        total = [total[c] - step * (roll(flux[c], -1, 0)[0:8] - flux[c][0:8]) for c in range(6)]
        change = [ahead[c][0:8] + fluxes[1, c, here, 0:8] for c in range(6)]
        left = corrected([upper[2, c, here, 0:8] for c in range(6)], change)
        right = corrected([lower[2, c, here, 0:8] for c in range(6)], change)
        flux = hllc_flux([roll(item, 1, 1) for item in left], right, 3)
        total = [total[c] - step * (roll(flux[c], -1, 1) - flux[c]) for c in range(6)]
        for c in range(6):
            out_ref[c, index] = total[c][:, 0:120]
        return jnp.maximum(fastest, jnp.where(lanes, fastest_signal(total), 0.0))

    fastest = lax.fori_loop(0, 4, final, jnp.zeros((8, 128), jnp.float32))
    signal_ref[...] = jnp.full(signal_ref.shape, jnp.max(fastest))


def hydro_step(column, by_even, own, by_odd, count):
    vmem = pl.BlockSpec(memory_space=pltpu.VMEM)
    blocks = [
        pltpu.with_memory_space_constraint(item, pltpu.VMEM)
        for item in (column, by_even, own, by_odd)
    ]
    return pl.pallas_call(
        kernel,
        in_specs=[vmem] * 4,
        out_specs=[vmem, vmem],
        out_shape=[
            pltpu.VMEM((6, 4, 8, 120), jnp.float32),
            pltpu.VMEM((count, 1, 1), jnp.float32),
        ],
        scratch_shapes=[
            pltpu.VMEM((6, 12, 16, 128), jnp.float32),
            pltpu.VMEM((3, 6, 6, 16, 128), jnp.float32),
            pltpu.VMEM((3, 6, 6, 16, 128), jnp.float32),
            pltpu.VMEM((3, 6, 6, 16, 128), jnp.float32),
            pltpu.VMEM((6, 5, 8, 128), jnp.float32),
        ],
        name="hydro",
    )(*blocks)


def cyclic(block, by_even, by_odd, odd):
    above, below = jnp.where(odd, by_odd, by_even), jnp.where(odd, by_even, by_odd)
    return jnp.concatenate([block, above, below], axis=2)


def step(conserved_state):
    tiles = lax.all_to_all(packed(conserved_state), PLANE, 0, 0, tiled=True)
    block, to_even, to_odd, to_column = unpacked(
        conserved_state, tiles, lax.axis_size(COLUMN)
    )
    x, chip_row, core = (lax.axis_index(axis) for axis in ("x", "zl", "c"))
    odd = x % 2 == 1
    far_second = (x == 0) | (x == lax.axis_size("x") - 1)
    far_first = ((core == 0) & (chip_row == 0)) | ((core == 1) & (chip_row == lax.axis_size("zl") - 1))
    beside_odd = swap(to_odd, GY, 1)
    ahead_odd = swap(block, GX, 1)
    column = over_column(to_column, 6)
    low, high = ahead_odd[:, :, :GHOST], ahead_odd[:, :, GHOST:]
    both = jnp.concatenate([to_even, jnp.where(odd, low, high)], axis=1)
    both = swap(both, GY, 0)
    beside_even, corner_even = both[:, :GHOST], both[:, GHOST:]
    kept = jnp.where(far_first, to_odd, beside_odd)
    corner_odd = lax.ppermute(
        jnp.where(far_second, kept, jnp.where(odd, high, low)), ALL, corner_swap()
    )
    own = cyclic(block, beside_even, beside_odd, odd)
    by_even = swap(own, GX, 0)
    corner_even, corner_odd, _ = lax.optimization_barrier((corner_even, corner_odd, own))
    by_odd = cyclic(ahead_odd, corner_even, corner_odd, odd)
    updated, to_plane = hydro_step(column, by_even, own, by_odd, lax.axis_size(PLANE))
    plane = lax.all_to_all(to_plane, PLANE, 0, 0, tiled=True)
    to_column = spread(plane, lax.axis_size(COLUMN))
    column = lax.all_to_all(to_column, COLUMN, 0, 0, tiled=True)
    return (updated, courant / jnp.max(column))


def solution(mesh):
    finer = Mesh(mesh.devices.reshape(16, 2, 2, 4, 4), ALL)
    spec = P(None, GX, GY, GZ)
    return jax.shard_map(step, mesh=finer, in_specs=(spec,), out_specs=(spec, P()), check_vma=False)
```

```python
import jax
import jax.numpy as jnp
from jax import lax
from jax.experimental import pallas as pl
from jax.experimental.pallas import tpu as pltpu
from jax.sharding import Mesh
from jax.sharding import PartitionSpec as P

GHOST = 4
ALL = ("zl", "c", "zh", "x", "y")
PLANE = ("c", "x", "y")
COLUMN = ("zl", "zh")
GX = ("zl", "c")
GY = ("zh", "x")
GZ = ("y",)

adiabatic = 5.0 / 3.0
courant = 0.3


def over_column(value, first):
    halves, rows = lax.axis_size("zh"), lax.axis_size("zl")
    deep = halves * rows
    order = [(first + step) % deep for step in range(deep)]
    columns, width = lax.axis_size("c"), lax.axis_size(("x", "y"))
    groups = [
        [(((z % rows) * columns + c) * halves + z // rows) * width + place for z in order]
        for c in range(columns)
        for place in range(width)
    ]
    return lax.all_to_all(value, ALL, 0, 0, axis_index_groups=groups, tiled=True)


def swaps(count):
    even = [(i, i ^ 1) for i in range(count)]
    odd = [(i, (i + 1) % count if i % 2 else (i - 1) % count) for i in range(count)]
    return even, odd


def swap(block, axes, odd):
    return lax.ppermute(block, axes, swaps(lax.axis_size(axes))[odd])


def corner_swap():
    sizes = [lax.axis_size(axis) for axis in ALL]
    rows, cores, halves, columns, width = sizes
    _, odd_first = swaps(rows * cores)
    _, odd_second = swaps(halves * columns)
    pairs = []
    for first in range(rows * cores):
        for second in range(halves * columns):
            far_first, far_second = first in (0, rows * cores - 1), second % columns in (0, columns - 1)
            to_first = odd_first[first][1] if far_second else first
            to_second = second if far_second and not far_first else odd_second[second][1]
            if far_first and not far_second:
                to_first = first
            for y in range(width):
                here = (first * halves * columns + second) * width + y
                there = (to_first * halves * columns + to_second) * width + y
                pairs.append((here, there))
    return pairs


def roll(value, shift, axis):
    return pltpu.roll(value, shift % value.shape[axis], axis)


def primitive_of(conserved):
    density, energy = conserved[0], conserved[4]
    inverse = 1.0 / density
    speed = [conserved[component] * inverse for component in (1, 2, 3)]
    kinetic = 0.5 * (conserved[1] * speed[0] + conserved[2] * speed[1] + conserved[3] * speed[2])
    return [density, *speed, (adiabatic - 1.0) * (energy - kinetic), conserved[5] * inverse]


def conserved_of(primitive):
    density = primitive[0]
    momenta = [density * primitive[component] for component in (1, 2, 3)]
    kinetic = 0.5 * (
        momenta[0] * primitive[1] + momenta[1] * primitive[2] + momenta[2] * primitive[3]
    )
    energy = primitive[4] * (1.0 / (adiabatic - 1.0)) + kinetic
    return [density, *momenta, energy, density * primitive[5]]


def fastest_signal(conserved):
    primitive = primitive_of(conserved)
    sound = jnp.sqrt(adiabatic * primitive[4] / primitive[0])
    speeds = jnp.maximum(
        jnp.maximum(jnp.abs(primitive[1]), jnp.abs(primitive[2])), jnp.abs(primitive[3])
    )
    return speeds + sound


def edge_of(q3, q2, q1, q, a1, a2):
    edge = (37.0 / 60.0) * (q1 + q) - (8.0 / 60.0) * (q2 + a1) + (1.0 / 60.0) * (q3 + a2)
    return jnp.clip(edge, jnp.minimum(q1, q), jnp.maximum(q1, q))


def limited(q, lower, upper):
    above, below = upper - q, q - lower
    spread = upper - lower
    skewed = spread * (0.5 * (below - above))
    limit = spread * spread * (1.0 / 6.0)
    flat = above * below <= 0.0
    new_lower = jnp.where(flat, q, jnp.where(skewed > limit, q - 2.0 * above, lower))
    new_upper = jnp.where(flat, q, jnp.where(skewed < -limit, q + 2.0 * below, upper))
    return new_lower, new_upper


def traced(primitive, edges, normal, half_step):
    slopes = [upper - lower for lower, upper in edges]
    density, speed, pressure = primitive[0], primitive[normal], primitive[4]
    rates = [-(speed * slopes[component]) for component in range(6)]
    rates[0] = rates[0] - density * slopes[normal]
    rates[normal] = rates[normal] - slopes[4] / density
    rates[4] = rates[4] - adiabatic * pressure * slopes[normal]
    moves = [half_step * rate for rate in rates]
    lower = [edges[component][0] + moves[component] for component in range(6)]
    upper = [edges[component][1] + moves[component] for component in range(6)]
    return lower, upper


def hllc_flux(left, right, normal):
    ratio_left, ratio_right = left[4] / left[0], right[4] / right[0]
    sound_left, sound_right = jnp.sqrt(adiabatic * ratio_left), jnp.sqrt(adiabatic * ratio_right)
    low = jnp.minimum(left[normal] - sound_left, right[normal] - sound_right)
    high = jnp.maximum(left[normal] + sound_left, right[normal] + sound_right)
    mass_left = left[0] * (low - left[normal])
    mass_right = right[0] * (high - right[normal])
    middle = (right[4] - left[4] + mass_left * left[normal] - mass_right * right[normal]) / (
        mass_left - mass_right
    )
    from_left = middle >= 0.0
    side = [jnp.where(from_left, left[component], right[component]) for component in range(6)]
    ratio = jnp.where(from_left, ratio_left, ratio_right)
    mass = jnp.where(from_left, mass_left, mass_right)
    outer = jnp.where(from_left, low, high)
    weight = jnp.where(from_left, jnp.minimum(low, 0.0), jnp.maximum(high, 0.0))
    speed, pressure = side[normal], side[4]
    state = conserved_of(side)
    flux = [item * speed for item in state]
    flux[normal] = flux[normal] + pressure
    flux[4] = flux[4] + pressure * speed
    factor = mass / (outer - middle)
    star = [factor * item for item in side]
    star[0] = factor
    star[normal] = factor * middle
    half_square = 0.5 * (side[1] * side[1] + side[2] * side[2] + side[3] * side[3])
    specific = ratio * (1.0 / (adiabatic - 1.0)) + half_square
    star[4] = factor * (specific + (middle - speed) * (middle + pressure / mass))
    return [flux[c] + weight * (star[c] - state[c]) for c in range(6)]


def maximum_of(everyone_ref):
    fastest = everyone_ref[0]
    for device in range(1, everyone_ref.shape[0]):
        fastest = jnp.maximum(fastest, everyone_ref[device])
    return fastest


def spread_kernel(everyone_ref, out_ref):
    out_ref[...] = jnp.broadcast_to(maximum_of(everyone_ref)[None], out_ref.shape)


def timestep_kernel(everyone_ref, out_ref):
    out_ref[...] = courant / maximum_of(everyone_ref)


def timestep(everyone):
    vmem = pl.BlockSpec(memory_space=pltpu.VMEM)
    return pl.pallas_call(
        timestep_kernel,
        in_specs=[vmem],
        out_specs=vmem,
        out_shape=jax.ShapeDtypeStruct((1, 1), jnp.float32),
        name="timestep",
    )(*in_vmem(everyone)).reshape(())


def spread(everyone, count):
    vmem = pl.BlockSpec(memory_space=pltpu.VMEM)
    return pl.pallas_call(
        spread_kernel,
        in_specs=[vmem],
        out_specs=vmem,
        out_shape=pltpu.VMEM((count, 1, 1), jnp.float32),
        name="spread",
    )(pltpu.with_memory_space_constraint(everyone, pltpu.VMEM))


def lane_ids():
    return lax.broadcasted_iota(jnp.int32, (8, 128), 1)


def pack_kernel(state_ref, out_ref, wide):
    lanes = lane_ids()
    for c in range(6):
        for layer in range(4):
            wide[c, layer, :, 0:120] = state_ref[c, layer]
    fastest = jnp.zeros((8, 128), jnp.float32)
    for layer in range(4):
        signal = fastest_signal([wide[c, layer] for c in range(6)])
        fastest = jnp.maximum(fastest, jnp.where(lanes < 120, signal, 0.0))
    first = last = jnp.full((8, 128), jnp.max(fastest))
    for c in range(6):
        for layer in range(4):
            spot = 4 * (4 * c + layer)
            here = (lanes >= spot) & (lanes < spot + 4)
            first = jnp.where(here, roll(wide[c, layer], spot, 1), first)
            last = jnp.where(here, roll(wide[c, layer], spot - 116, 1), last)
    above = lax.rem(lax.axis_index("y") + 1, 4)
    for y in range(4):
        tile = jnp.where(above == y, last, first)
        for place in range(y, 32, 4):
            out_ref[place] = tile


def unpack_kernel(state_ref, tiles_ref, block_ref, even_ref, odd_ref, column_ref):
    lanes = lane_ids()
    fastest = tiles_ref[0]
    for place in range(1, 32):
        fastest = jnp.maximum(fastest, tiles_ref[place])
    fastest = jnp.max(jnp.where(lanes >= 96, fastest, 0.0))
    column_ref[...] = jnp.full(column_ref.shape, fastest)
    y = lax.axis_index("y")
    base = 16 * lax.axis_index("c") + 4 * lax.axis_index("x")
    odd = lax.rem(lax.axis_index("x"), 2) == 1
    below = tiles_ref[base + lax.rem(y + 3, 4)]
    above = tiles_ref[base + lax.rem(y + 1, 4)]
    for c in range(6):
        for layer in range(4):
            spot = 4 * (4 * c + layer)
            ghosts = jnp.where(lanes < 124, roll(above, 120 - spot, 1), roll(below, 124 - spot, 1))
            block_ref[c, layer] = ghosts
            block_ref[c, layer, :, 0:120] = state_ref[c, layer]
            whole = block_ref[c, layer]
            first, last = whole[0:4], whole[4:8]
            even_ref[c, layer] = jnp.where(odd, first, last)
            odd_ref[c, layer] = jnp.where(odd, last, first)


def in_vmem(*arrays):
    return [pltpu.with_memory_space_constraint(item, pltpu.VMEM) for item in arrays]


def packed(state):
    vmem = pl.BlockSpec(memory_space=pltpu.VMEM)
    return pl.pallas_call(
        pack_kernel,
        in_specs=[vmem],
        out_specs=vmem,
        out_shape=jax.ShapeDtypeStruct((32, 8, 128), jnp.float32),
        scratch_shapes=[pltpu.VMEM((6, 4, 8, 128), jnp.float32)],
        name="pack",
    )(*in_vmem(state))


def unpacked(state, tiles, count):
    vmem = pl.BlockSpec(memory_space=pltpu.VMEM)
    return pl.pallas_call(
        unpack_kernel,
        in_specs=[vmem] * 2,
        out_specs=[vmem] * 4,
        out_shape=[
            pltpu.VMEM((6, 4, 8, 128), jnp.float32),
            pltpu.VMEM((6, 4, 4, 128), jnp.float32),
            pltpu.VMEM((6, 4, 4, 128), jnp.float32),
            jax.ShapeDtypeStruct((count, 1, 1), jnp.float32),
        ],
        name="unpack",
    )(*in_vmem(state, tiles))


def kernel(column_ref, even_ref, own_ref, odd_ref, out_ref, signal_ref, prim, lower, upper, fluxes, gx):
    step = jnp.max(courant / maximum_of(column_ref))
    half = 0.5 * step
    even_start = 8 - 8 * lax.axis_index("c")
    for source, start in ((even_ref, even_start), (own_ref, 4), (odd_ref, 8 - even_start)):
        for layer in range(4):
            values = primitive_of([source[c, layer] for c in range(6)])
            for c in range(6):
                prim[c, start + layer] = values[c]

    def faces(index, carry):
        own = [prim[c, index + 3] for c in range(6)]
        edges = []
        for c in range(6):
            q = [prim[c, index + k] for k in range(7)]
            edges.append(
                limited(own[c], edge_of(*q[0:6]), edge_of(*q[1:7]))
            )
        for axis in range(3):
            if axis:
                edges = []
                for c in range(6):
                    q = own[c]
                    near = [roll(q, k, axis - 1) for k in (3, 2, 1)]
                    far = [roll(q, -k, axis - 1) for k in (1, 2)]
                    edge = edge_of(*near, q, *far)
                    edges.append(limited(q, edge, roll(edge, -1, axis - 1)))
            low_face, high_face = traced(own, edges, 1 + axis, half)
            for c in range(6):
                lower[axis, c, index] = low_face[c]
                upper[axis, c, index] = high_face[c]
        return carry

    lax.fori_loop(0, 6, faces, 0)

    def predicted(index, carry):
        for axis in (1, 2):
            left = [roll(upper[axis, c, index], 1, axis - 1) for c in range(6)]
            flux = hllc_flux(left, [lower[axis, c, index] for c in range(6)], 1 + axis)
            for c in range(6):
                fluxes[axis, c, index] = half * (roll(flux[c], -1, axis - 1) - flux[c])
        return carry

    lax.fori_loop(0, 6, predicted, 0)

    def predicted_first(index, carry):
        flux = hllc_flux(
            [upper[0, c, index] for c in range(6)], [lower[0, c, index + 1] for c in range(6)], 1
        )
        for c in range(6):
            fluxes[0, c, index] = flux[c]
        return carry

    lax.fori_loop(0, 5, predicted_first, 0)

    def corrected(states, changes):
        state = conserved_of(states)
        return primitive_of([state[c] - changes[c] for c in range(6)])

    def final_first(index, carry):
        change = [fluxes[1, c, index + 1, 0:8] + fluxes[2, c, index + 1, 0:8] for c in range(6)]
        before = [carry[c] for c in range(6)]
        right = corrected([lower[0, c, index + 1, 0:8] for c in range(6)], change)
        flux = hllc_flux(before, right, 1)
        for c in range(6):
            gx[c, index] = flux[c]
        return tuple(corrected([upper[0, c, index + 1, 0:8] for c in range(6)], change))

    change = [fluxes[1, c, 0, 0:8] + fluxes[2, c, 0, 0:8] for c in range(6)]
    first = tuple(corrected([upper[0, c, 0, 0:8] for c in range(6)], change))
    lax.fori_loop(0, 5, final_first, first)

    lanes = lane_ids() < 120

    def final(index, fastest):
        here = index + 1
        total = [own_ref[c, index, 0:8] - step * (gx[c, index + 1] - gx[c, index]) for c in range(6)]
        ahead = [half * (fluxes[0, c, here] - fluxes[0, c, index]) for c in range(6)]
        change = [ahead[c] + fluxes[2, c, here] for c in range(6)]
        left = corrected([upper[1, c, here] for c in range(6)], change)
        right = corrected([lower[1, c, here] for c in range(6)], change)
        flux = hllc_flux([roll(item, 1, 0) for item in left], right, 2)
        total = [total[c] - step * (roll(flux[c], -1, 0)[0:8] - flux[c][0:8]) for c in range(6)]
        change = [ahead[c][0:8] + fluxes[1, c, here, 0:8] for c in range(6)]
        left = corrected([upper[2, c, here, 0:8] for c in range(6)], change)
        right = corrected([lower[2, c, here, 0:8] for c in range(6)], change)
        flux = hllc_flux([roll(item, 1, 1) for item in left], right, 3)
        total = [total[c] - step * (roll(flux[c], -1, 1) - flux[c]) for c in range(6)]
        for c in range(6):
            out_ref[c, index] = total[c][:, 0:120]
        return jnp.maximum(fastest, jnp.where(lanes, fastest_signal(total), 0.0))

    fastest = lax.fori_loop(0, 4, final, jnp.zeros((8, 128), jnp.float32))
    signal_ref[...] = jnp.full(signal_ref.shape, jnp.max(fastest))


def hydro_step(column, by_even, own, by_odd, count):
    vmem = pl.BlockSpec(memory_space=pltpu.VMEM)
    blocks = [
        pltpu.with_memory_space_constraint(item, pltpu.VMEM)
        for item in (column, by_even, own, by_odd)
    ]
    return pl.pallas_call(
        kernel,
        in_specs=[vmem] * 4,
        out_specs=[vmem, vmem],
        out_shape=[
            pltpu.VMEM((6, 4, 8, 120), jnp.float32),
            pltpu.VMEM((count, 1, 1), jnp.float32),
        ],
        scratch_shapes=[
            pltpu.VMEM((6, 12, 16, 128), jnp.float32),
            pltpu.VMEM((3, 6, 6, 16, 128), jnp.float32),
            pltpu.VMEM((3, 6, 6, 16, 128), jnp.float32),
            pltpu.VMEM((3, 6, 6, 16, 128), jnp.float32),
            pltpu.VMEM((6, 5, 8, 128), jnp.float32),
        ],
        name="hydro",
    )(*blocks)


def cyclic(block, by_even, by_odd, odd):
    above, below = jnp.where(odd, by_odd, by_even), jnp.where(odd, by_even, by_odd)
    return jnp.concatenate([block, above, below], axis=2)


def step(conserved_state):
    tiles = lax.all_to_all(packed(conserved_state), PLANE, 0, 0, tiled=True)
    block, to_even, to_odd, to_column = unpacked(
        conserved_state, tiles, lax.axis_size(COLUMN)
    )
    x, chip_row, core = (lax.axis_index(axis) for axis in ("x", "zl", "c"))
    odd = x % 2 == 1
    far_second = (x == 0) | (x == lax.axis_size("x") - 1)
    far_first = ((core == 0) & (chip_row == 0)) | ((core == 1) & (chip_row == lax.axis_size("zl") - 1))
    beside_odd = swap(to_odd, GY, 1)
    ahead_odd = swap(block, GX, 1)
    column = over_column(to_column, 8)
    low, high = ahead_odd[:, :, :GHOST], ahead_odd[:, :, GHOST:]
    both = jnp.concatenate([to_even, jnp.where(odd, low, high)], axis=1)
    both = swap(both, GY, 0)
    beside_even, corner_even = both[:, :GHOST], both[:, GHOST:]
    kept = jnp.where(far_first, to_odd, beside_odd)
    corner_odd = lax.ppermute(
        jnp.where(far_second, kept, jnp.where(odd, high, low)), ALL, corner_swap()
    )
    own = cyclic(block, beside_even, beside_odd, odd)
    by_even = swap(own, GX, 0)
    corner_even, corner_odd, _ = lax.optimization_barrier((corner_even, corner_odd, own))
    by_odd = cyclic(ahead_odd, corner_even, corner_odd, odd)
    updated, to_plane = hydro_step(column, by_even, own, by_odd, lax.axis_size(PLANE))
    plane = lax.all_to_all(to_plane, PLANE, 0, 0, tiled=True)
    to_column = spread(plane, lax.axis_size(COLUMN))
    column = lax.all_to_all(to_column, COLUMN, 0, 0, tiled=True)
    return (updated, timestep(column))


def solution(mesh):
    finer = Mesh(mesh.devices.reshape(16, 2, 2, 4, 4), ALL)
    spec = P(None, GX, GY, GZ)
    return jax.shard_map(step, mesh=finer, in_specs=(spec,), out_specs=(spec, P()), check_vma=False)
```
